32 devices in a mesh: row: 8 (over y, x, core), col: 4 (over z).
Axes of the slice: x: 2, y: 2, z: 4, core: 2. Of those that a mesh axis runs over, the one named last changes fastest.
Arguments:
- expression: bfloat16 [4096, 1024], P(('row', 'col')), may hold values from -200 to 200, as said below
- powers: int32 [10], replicated, may hold values from 1 to 20
Outputs:
- log_degree: float32 [10, 4096], P(None, ('row', 'col'))
- degree_freq: float32 [10, 10], replicated
- fit_slope: float32 [10], replicated
- mean_log: float32 [10], replicated
The draws below stay inside these ranges and needn't reach their ends.
Inputs may be any that keep to these rules, and one draw needn't show every extreme that they name: Finite expression values.
All inputs are finite; a program needn't handle non-finite values.
Results may differ from the reference program's by a relative error of at most 0.0003.
Values may be sent and summed in bfloat16 or wider, within the bound.
A program may use at most 64 MiB of HBM per device.

```python
import math
import jax
import jax.numpy as jnp
from jax import lax

S = 1024
NPOW = 10
BINS = 10
MODULES = 400
GENES = 4096


def draw_expression(key, part):
    keys = jax.random.split(key, 10)
    leading_count = max(MODULES // 8, 1)
    leading_ids = jax.random.randint(keys[0], (GENES, 1), 0, leading_count)
    other_ids = jax.random.randint(keys[8], (GENES, 7), 0, MODULES)
    factor_ids = jnp.concatenate([leading_ids, other_ids], axis=1)
    live_count = jax.random.randint(keys[1], (GENES, 1), 1, 6)
    slot_index = jnp.arange(8, dtype=jnp.int32)[None, :]
    leading_strength = jax.random.uniform(keys[2], (GENES, 1), jnp.float32, 0.85, 1.0)
    other_strength = jax.random.uniform(keys[9], (GENES, 7), jnp.float32, 0.1, 0.3)
    strength = jnp.concatenate([leading_strength, other_strength], axis=1)
    signs = (jax.random.randint(keys[3], (GENES, 8), 0, 2) * 2 - 1).astype(jnp.float32)
    loading = jnp.where(slot_index < live_count, strength * signs, 0.0)
    factors = jax.random.normal(keys[4], (MODULES, S), jnp.float32)
    signal = jnp.zeros((GENES, S), jnp.float32)
    for slot in range(8):
        signal = signal + loading[:, slot:slot + 1] * jnp.take(factors, factor_ids[:, slot], axis=0)
    noise_scale = jnp.exp(jax.random.uniform(keys[5], (GENES, 1), jnp.float32, -3.0, 1.0))
    noise_part = jax.random.normal(keys[6], (GENES, S), jnp.float32)
    total = jnp.sum(loading * loading, axis=1, keepdims=True) + noise_scale * noise_scale
    values = (signal + noise_scale * noise_part) / jnp.sqrt(total)
    return values.astype(jnp.bfloat16)


def place_ends(result, own_key, least, top_value):
    shape = result.shape
    spot = [jax.random.randint(jax.random.fold_in(own_key, axis), (), 0, shape[axis]) for axis in range(len(shape))]
    result = result.at[tuple(spot)].set(least)
    longest = shape.index(max(shape))
    spot[longest] = (spot[longest] + 1) % shape[longest]
    return result.at[tuple(spot)].set(top_value)


def setup_inputs(seed: int = 0) -> dict:
    arg_keys = jax.random.split(jax.random.key(seed), 3)
    expression = draw_expression(jax.random.fold_in(arg_keys[2], 71), 0)
    powers = place_ends(jax.random.randint(arg_keys[1], (NPOW,), 1, 21), jax.random.fold_in(arg_keys[1], 1), 1, 20).astype(jnp.int32)
    return dict(expression=expression, powers=powers)


def reference(expression, powers):
    values = expression.astype(jnp.float32)
    gene_mean = lax.optimization_barrier(jnp.mean(values, axis=1))
    centred = values - gene_mean[:, None]
    gene_inv = lax.rsqrt(lax.optimization_barrier(jnp.mean(centred * centred, axis=1)) + 1e-06)
    exponents = powers.astype(jnp.float32)
    block_rows = math.gcd(GENES, 512)
    blocks = GENES // block_rows

    def one_block(packed):
        row_block, block_mean, block_inv = packed
        raw = jnp.dot(row_block, expression.T, preferred_element_type=jnp.float32)
        pearson = (raw / S - block_mean[:, None] * gene_mean[None, :]) * block_inv[:, None] * gene_inv[None, :]
        log_abs = jnp.log(jnp.abs(pearson))
        return jnp.stack([lax.optimization_barrier(jnp.sum(jnp.exp(exponents[power_index] * log_abs), axis=1)) for power_index in range(NPOW)])
    blocked = lax.map(one_block, (expression.reshape(blocks, block_rows, S), gene_mean.reshape(blocks, block_rows), gene_inv.reshape(blocks, block_rows)))
    degree = jnp.transpose(blocked, (1, 0, 2)).reshape(NPOW, GENES)
    peak = lax.optimization_barrier(jnp.max(degree, axis=1))
    position = jnp.clip(BINS * degree / peak[:, None] - 0.5, 0.0, BINS - 1.0)
    centres = jnp.arange(BINS, dtype=jnp.float32)
    weights = jnp.maximum(0.0, 1.0 - jnp.abs(position[:, :, None] - centres[None, None, :]))
    degree_freq = lax.optimization_barrier(jnp.sum(weights, axis=1)) / GENES
    mean_log = jnp.log10(lax.optimization_barrier(jnp.sum(degree, axis=1)) / GENES)
    xfit = jnp.log10((centres[None, :] + 0.5) * peak[:, None] / BINS)
    yfit = jnp.log10(degree_freq + 1.0 / GENES)
    xdev = xfit - lax.optimization_barrier(jnp.mean(xfit, axis=1, keepdims=True))
    ydev = yfit - lax.optimization_barrier(jnp.mean(yfit, axis=1, keepdims=True))
    fit_slope = lax.optimization_barrier(jnp.sum(xdev * ydev, axis=1)) / lax.optimization_barrier(jnp.sum(xdev * xdev, axis=1))
    return (jnp.log10(degree), degree_freq, fit_slope, mean_log)
```

```python
import functools
import math

import jax
import jax.numpy as jnp
from jax import lax
from jax.experimental import pallas as pl
from jax.experimental.pallas import tpu as pltpu
from jax.sharding import PartitionSpec as P

BINS = 10
EDGES = (0, 2, 4, 6, 7, 8)
CHUNKS = len(EDGES) - 1
LATE = 3
STATS = CHUNKS
STRIP = 32
LOG2E = math.log2(math.e)
LOG10E = math.log10(math.e)
MESH = pl.DeviceIdType.MESH


def split(size):
    low = max(f for f in range(1, math.isqrt(size) + 1) if size % f == 0)
    return size // low, low


def kernel(
    n0, n1, nh, nl, npower, powers_hbm, expr_hbm, log_degree_ref, fit_ref,
    powers_ref, left, right, stats, right_mean, right_inv, raw_ref, sums_ref, partial, degrees,
    load_sem, far_send, side_send, near_send, up_send, twin_send, stat_send,
    far_recv, side_recv, near_recv, up_recv, twin_recv, stat_recv, part_sem, deg_sem,
):
    r, c = lax.axis_index("row"), lax.axis_index("col")
    q, core = r // 2, r % 2
    q1, q0 = q // n0, q % n0
    ch, cl = c // nl, c % nl
    nleft, npair = nh * n0, nl * n1
    _, genes, samples = left.shape
    edges = [genes * e // EDGES[-1] for e in EDGES]
    late = 2 * edges[LATE]

    def device(d0=0, dh=0, d1=0, dl=0, other=False):
        row = (((q1 + d1) % n1) * n0 + (q0 + d0) % n0) * 2 + (1 - core if other else core)
        return row, ((ch + dh) % nh) * nl + (cl + dl) % nl

    def left_slot(dh, d0):
        return ((ch + nh - dh) % nh) * n0 + (q0 + n0 - d0) % n0

    def pair_slot(dl, d1):
        return ((cl + nl - dl) % nl) * n1 + (q1 + n1 - d1) % n1

    own_left, own_pair = left_slot(0, 0), pair_slot(0, 0)
    block = left.at[own_left]

    def left_piece(slot, k):
        if k == STATS:
            return stats.at[slot]
        return left.at[slot, pl.ds(edges[k], edges[k + 1] - edges[k])]

    def right_piece(slot, side, k):
        if k == STATS:
            return stats.at[nleft + slot * 2 + side]
        size = edges[k + 1] - edges[k]
        return right.at[slot, pl.ds(2 * edges[k] + side * size, size)]

    loads = [
        pltpu.make_async_copy(expr_hbm, block, load_sem.at[0]),
        pltpu.make_async_copy(powers_hbm, powers_ref, load_sem.at[1]),
    ]
    for load in loads:
        load.start()
    for k in range(CHUNKS):
        source = expr_hbm.at[pl.ds(edges[k], edges[k + 1] - edges[k])]
        pltpu.make_async_copy(source, right_piece(own_pair, core, k), load_sem.at[2]).start()

    barrier = pltpu.get_barrier_semaphore()
    greeted = [dict(other=True)]
    greeted += [dict(d0=d) for d in range(1, n0)]
    greeted += [dict(d1=d) for d in range(1, n1)]
    greeted += [dict(dh=d) for d in range(1, nh)]
    greeted += [dict(dl=d) for d in range(1, nl)]
    for where in greeted:
        pl.semaphore_signal(barrier, inc=1, device_id=device(**where), device_id_type=MESH)

    loads.append(pltpu.make_async_copy(expr_hbm, block, load_sem.at[2]))
    for load in loads:
        load.wait()

    values = left[own_left].astype(jnp.float32)
    mean = jnp.mean(values, axis=1, keepdims=True)
    centred = values - mean
    inv = lax.rsqrt(jnp.mean(centred * centred, axis=1, keepdims=True) + 1e-06)
    own_stats = jnp.concatenate(
        [jnp.broadcast_to(mean, (genes, 128)).T[0:1, :], jnp.broadcast_to(inv, (genes, 128)).T[0:1, :]], axis=0
    )
    stats[own_left] = own_stats
    stats[nleft + own_pair * 2 + core] = own_stats
    for slot in range(nleft):
        for p in range(npower):
            sums_ref[slot, p] = jnp.zeros((8, genes), jnp.float32)
    exponents = [powers_ref[p].astype(jnp.float32) * LOG2E for p in range(npower)]

    pl.semaphore_wait(barrier, len(greeted))

    def remote(ref, send, recv, where):
        return pltpu.make_async_remote_copy(
            src_ref=ref, dst_ref=ref, send_sem=send, recv_sem=recv, device_id=device(**where), device_id_type=MESH
        )

    flows = [("far", dh, 0) for dh in range(1, nh)] + [("near", dl, 0) for dl in range(1, nl)]
    flows += [("side", dh, d0) for dh in range(nh) for d0 in range(1, n0)]
    flows += [("up", dl, d1) for dl in range(nl) for d1 in range(1, n1)]
    flows += [("twin", dl, d1) for dl in range(nl) for d1 in range(n1)]

    def sems(kind, a, b, k):
        if k == STATS:
            return stat_send.at[0], stat_recv.at[flows.index((kind, a, b))]
        if kind == "far":
            return far_send.at[a - 1], far_recv.at[a - 1, k]
        if kind == "near":
            return near_send.at[a - 1], near_recv.at[a - 1, k]
        if kind == "side":
            return side_send.at[a, b - 1], side_recv.at[a, b - 1]
        if kind == "up":
            return up_send.at[a, b - 1], up_recv.at[a, b - 1, k]
        return twin_send.at[a, b], twin_recv.at[a, b, int(k >= LATE)]

    def send(kind, a, b, k):
        if kind == "far":
            ref, where = left_piece(own_left, k), dict(dh=a)
        elif kind == "side":
            ref, where = left_piece(left_slot(a, 0), k), dict(d0=b)
        elif kind == "near":
            ref, where = right_piece(own_pair, core, k), dict(dl=a)
        elif kind == "up":
            ref, where = right_piece(pair_slot(a, 0), core, k), dict(d1=b)
        else:
            ref, where = right_piece(pair_slot(a, b), core, k), dict(other=True)
        remote(ref, *sems(kind, a, b, k), where).start()

    def wait(kind, a, b, k, ref):
        remote(ref, *sems(kind, a, b, k), dict(other=True)).wait_recv()

    def wait_far(dh, k):
        wait("far", dh, 0, k, left_piece(left_slot(dh, 0), k))

    def wait_side(dh, d0, k):
        wait("side", dh, d0, k, left_piece(left_slot(dh, d0), k) if k == STATS else left.at[left_slot(dh, d0)])

    def wait_near(dl, k):
        wait("near", dl, 0, k, right_piece(pair_slot(dl, 0), core, k))

    def wait_up(dl, d1, k):
        wait("up", dl, d1, k, right_piece(pair_slot(dl, d1), core, k))

    def wait_twin(dl, d1, k):
        slot = pair_slot(dl, d1)
        if k == STATS:
            ref = right_piece(slot, 1 - core, k)
        else:
            ref = right.at[slot, pl.ds(0, edges[LATE]) if k < LATE else pl.ds(late, genes - edges[LATE])]
        wait("twin", dl, d1, k, ref)

    for k in (STATS, *range(CHUNKS)):
        for first in (0, 1):
            @pl.when(core == first)
            def _():
                for kind in ("far", "near") if first == 0 else ("near", "far"):
                    for a in range(1, nh if kind == "far" else nl):
                        send(kind, a, 0, k)

        for d0 in range(1, n0):
            send("side", 0, d0, k)
        for d1 in range(1, n1):
            send("up", 0, d1, k)
        send("twin", 0, 0, k)

    def multiply(ls, blocks, ps, pairs, lo=0, hi=2 * genes):
        size = hi - lo
        lhs = right[pl.ds(ps, pairs), lo:hi].reshape(pairs * size, samples)
        rhs = left[pl.ds(ls, blocks)].reshape(blocks * genes, samples)
        raw = lax.dot_general(lhs, rhs, (((1,), (1,)), ((), ())), preferred_element_type=jnp.float32)
        for a in range(blocks):
            for b in range(pairs):
                raw_ref[ls + a, ps + b, lo:hi] = raw[b * size:(b + 1) * size, a * genes:(a + 1) * genes]

    def accumulate(ls, ps, lo=0, hi=2 * genes):
        mean_row, inv_row = stats[ls, 0:1, :], stats[ls, 1:2, :]
        totals = [None] * npower
        for s in range(lo, hi, STRIP):
            raw = raw_ref[ls, ps, s:s + STRIP, :]
            mean_col, inv_col = right_mean[ps, s:s + STRIP, :], right_inv[ps, s:s + STRIP, :]
            pearson = (raw * (1.0 / samples) - mean_col * mean_row) * inv_col * inv_row
            log_abs = jnp.log(jnp.abs(pearson))
            for p in range(npower):
                part = jnp.sum(jnp.exp2(exponents[p] * log_abs).reshape(STRIP // 8, 8, genes), axis=0)
                totals[p] = part if totals[p] is None else totals[p] + part
        for p in range(npower):
            sums_ref[ls, p] = sums_ref[ls, p] + totals[p]

    def run(ls, blocks, ps, pairs, lo=0, hi=2 * genes):
        multiply(ls, blocks, ps, pairs, lo, hi)

        def body(u, _):
            accumulate(ls + lax.rem(u, blocks), ps + lax.div(u, blocks), lo, hi)
            return 0

        lax.fori_loop(0, blocks * pairs, body, 0)

    def columns(dl, d1):
        slot = pair_slot(dl, d1)
        for side in (0, 1):
            row = stats[nleft + slot * 2 + side]
            mean_col = jnp.broadcast_to(row[0:1], (128, genes)).T
            inv_col = jnp.broadcast_to(row[1:2], (128, genes)).T
            for k in range(CHUNKS):
                low, high = edges[k], edges[k + 1]
                window = pl.ds(2 * low + side * (high - low), high - low)
                right_mean[slot, window] = mean_col[low:high]
                right_inv[slot, window] = inv_col[low:high]

    own_row, own_line = ch * n0, cl * n1
    far_pairs = [(dl, 0) for dl in range(1, nl)]
    rest_pairs = [(dl, d1) for dl in range(1, nl) for d1 in range(1, n1)]
    far_rows = [(ch + nh - dh) % nh * n0 for dh in range(1, nh)]
    far_blocks = [left_slot(dh, 0) for dh in range(1, nh)]
    rest_blocks = [(dh, d0) for dh in range(1, nh) for d0 in range(1, n0)]

    def pass_up(k):
        for d1 in range(1, n1):
            wait_up(0, d1, k)
            send("twin", 0, d1, k)

    def pass_far(k):
        for dl in range(1, nl):
            wait_near(dl, k)
            for d1 in range(1, n1):
                send("up", dl, d1, k)
            send("twin", dl, 0, k)
        for dh in range(1, nh):
            wait_far(dh, k)
            for d0 in range(1, n0):
                send("side", dh, d0, k)

    def pass_rest(k):
        for dl, d1 in rest_pairs:
            wait_up(dl, d1, k)
            send("twin", dl, d1, k)

    wait_twin(0, 0, STATS)
    wait_twin(0, 0, 0)
    wait_twin(0, 0, LATE)
    columns(0, 0)
    pass_up(STATS)
    pass_far(STATS)
    pass_up(0)
    pass_up(1)
    pass_far(0)
    pass_rest(STATS)
    pass_up(2)
    pass_up(3)
    for dl in range(nl):
        for d1 in range(n1):
            if dl or d1:
                wait_twin(dl, d1, STATS)
                columns(dl, d1)
    for dh in range(nh):
        for d0 in range(1, n0):
            wait_side(dh, d0, STATS)
    pass_up(4)
    pass_far(1)
    for d0 in range(1, n0):
        wait_side(0, d0, 0)
    run(own_row, n0, own_pair, 1)
    pass_rest(0)
    for d1 in range(1, n1):
        wait_twin(0, d1, 0)
        wait_twin(0, d1, LATE)
        run(own_row, n0, pair_slot(0, d1), 1)
    pass_far(2)
    pass_rest(1)
    pass_far(3)
    for dl, d1 in far_pairs:
        wait_twin(dl, d1, 0)
        run(own_row, n0, pair_slot(dl, d1), 1, 0, late)
    pass_far(4)
    for b in far_blocks:
        run(b, 1, own_line, n1)
    pass_rest(2)
    for dl, d1 in far_pairs:
        wait_twin(dl, d1, LATE)
        for b in far_blocks:
            run(b, 1, pair_slot(dl, d1), 1)
        run(own_row, n0, pair_slot(dl, d1), 1, late)
    pass_rest(3)
    pass_rest(4)
    for dh, d0 in rest_blocks:
        wait_side(dh, d0, 0)
        run(left_slot(dh, d0), 1, own_line, n1)
        for m in far_pairs:
            run(left_slot(dh, d0), 1, pair_slot(*m), 1)
    for dl, d1 in rest_pairs:
        wait_twin(dl, d1, 0)
        wait_twin(dl, d1, LATE)
        run(0, nleft, pair_slot(dl, d1), 1)

    height = partial.shape[1]
    lines = [
        jnp.sum(sums_ref[slot, p], axis=0, keepdims=True) for slot in range(nleft) for p in range(npower)
    ]
    if height > nleft * npower:
        lines.append(jnp.zeros((height - nleft * npower, genes), jnp.float32))
    partial[own_left] = jnp.concatenate(lines, axis=0)

    mine_part = partial.at[own_left]
    for dh in reversed(range(nh)):
        for d0 in reversed(range(n0)):
            if dh or d0:
                remote(mine_part, part_sem.at[0], part_sem.at[1], dict(dh=dh, d0=d0)).start()
    others = partial.at[pl.ds(0, nleft - 1)]
    remote(others, part_sem.at[0], part_sem.at[1], dict(other=True)).wait_recv()
    total = partial[0]
    for slot in range(1, nleft):
        total = total + partial[slot]
    own = own_pair * 2 + core
    degrees[own] = total

    for dl in reversed(range(nl)):
        for d1 in reversed(range(n1)):
            for o in (True, False):
                if dl or d1 or o:
                    remote(degrees.at[own], deg_sem.at[0], deg_sem.at[1], dict(dl=dl, d1=d1, other=o)).start()
    mine = total[:npower]
    for slot in range(1, nleft):
        mine = jnp.where(own_left == slot, total[slot * npower:(slot + 1) * npower], mine)
    log_degree_ref[...] = jnp.log(mine) * LOG10E

    for kind, a, b in flows:
        remote(block, *sems(kind, a, b, 0), dict(other=True)).wait_send()
    remote(stats.at[pl.ds(0, len(flows))], *sems(*flows[0], STATS), dict(other=True)).wait_send()
    remote(others, part_sem.at[0], part_sem.at[1], dict(other=True)).wait_send()
    rest = degrees.at[pl.ds(0, 2 * npair - 1)]
    remote(rest, deg_sem.at[0], deg_sem.at[1], dict(other=True)).wait_recv()
    fit(genes * nleft * npair * 2, nleft, npower, degrees, fit_ref)
    remote(rest, deg_sem.at[0], deg_sem.at[1], dict(other=True)).wait_send()


def fit(genes_all, nleft, npower, degrees, fit_ref):
    blocks, height, genes = degrees.shape
    padded = npower + 8 - npower % 8
    spare = height - nleft * npower

    def fold(values, combine):
        total = values[:npower]
        for block in range(1, nleft):
            total = combine(total, values[block * npower:(block + 1) * npower])
        return jnp.concatenate([total, jnp.ones((padded - npower, 1), jnp.float32)], axis=0)

    best = lax.fori_loop(1, blocks, lambda index, best: jnp.maximum(best, degrees[index]), degrees[0])
    peak = fold(jnp.max(best, axis=1, keepdims=True), jnp.maximum)
    scales = [(BINS / peak)[:npower]] * nleft
    if spare:
        scales.append(jnp.ones((spare, 1), jnp.float32))
    scale = jnp.broadcast_to(jnp.concatenate(scales, axis=0), (height, genes))

    def weigh(index, carry):
        carry = list(carry)
        degree = degrees[index]
        position = jnp.clip(degree * scale - 0.5, 0.0, BINS - 1.0)
        for b in range(BINS):
            carry[b] = carry[b] + jnp.maximum(0.0, 1.0 - jnp.abs(position - b))
        carry[BINS] = carry[BINS] + degree
        return tuple(carry)

    totals = lax.fori_loop(0, blocks, weigh, tuple(jnp.zeros((height, genes), jnp.float32) for _ in range(BINS + 1)))
    totals = [fold(jnp.sum(total, axis=1, keepdims=True), jnp.add) for total in totals]
    lane = lax.broadcasted_iota(jnp.int32, (padded, 128), 1)
    line = lax.broadcasted_iota(jnp.int32, (padded, 128), 0)
    freq = jnp.zeros((padded, 128), jnp.float32)
    for b in range(BINS):
        freq = jnp.where(lane == b, totals[b], freq)
    freq = freq / genes_all
    fit_ref[0:padded, :] = freq
    mean_log = jnp.log(totals[BINS] / genes_all) * LOG10E
    inside = lane < BINS
    xfit = jnp.log((lane.astype(jnp.float32) + 0.5) * peak / BINS) * LOG10E
    yfit = jnp.log(freq + 1.0 / genes_all) * LOG10E

    def deviation(values):
        mean = jnp.sum(jnp.where(inside, values, 0.0), axis=1, keepdims=True) / BINS
        return jnp.where(inside, values - mean, 0.0)

    xdev, ydev = deviation(xfit), deviation(yfit)
    slope = jnp.sum(xdev * ydev, axis=1, keepdims=True) / jnp.sum(xdev * xdev, axis=1, keepdims=True)
    on_line = jnp.logical_and(lane == line, line < npower)
    fit_ref[padded:padded + 1, :] = jnp.sum(jnp.where(on_line, slope, 0.0), axis=0, keepdims=True)
    fit_ref[padded + 1:padded + 2, :] = jnp.sum(jnp.where(on_line, mean_log, 0.0), axis=0, keepdims=True)


def unpack_kernel(npower, log_degree_in, fit_in, log_degree_ref, freq_ref, slope_ref, mean_log_ref):
    padded = fit_in.shape[0] - 8
    log_degree_ref[...] = log_degree_in[...]
    freq_ref[...] = fit_in[0:npower, :BINS]
    slope_ref[...] = fit_in[padded:padded + 1, :npower]
    mean_log_ref[...] = fit_in[padded + 1:padded + 2, :npower]


def solution(mesh):
    nr, nc = mesh.shape["row"], mesh.shape["col"]
    n1, n0 = split(nr // 2)
    nh, nl = split(nc)

    def on_device(expression, powers):
        genes, samples = expression.shape
        npower = powers.shape[0]
        nleft, npair = nh * n0, nl * n1
        height = -(-npower * nleft // 8) * 8
        vmem = pl.BlockSpec(memory_space=pltpu.VMEM)
        hbm = pl.BlockSpec(memory_space=pltpu.HBM)
        dma = pltpu.SemaphoreType.DMA
        f32 = jnp.float32
        padded = npower + 8 - npower % 8
        log_degree, packed = pl.pallas_call(
            functools.partial(kernel, n0, n1, nh, nl, npower),
            out_shape=(
                jax.ShapeDtypeStruct((npower, genes), f32),
                jax.ShapeDtypeStruct((padded + 8, 128), f32),
            ),
            in_specs=[hbm, hbm],
            out_specs=(vmem, vmem),
            scratch_shapes=[
                pltpu.SMEM((npower,), jnp.int32),
                pltpu.VMEM((nleft, genes, samples), jnp.bfloat16),
                pltpu.VMEM((npair, 2 * genes, samples), jnp.bfloat16),
                pltpu.VMEM((nleft + 2 * npair, 2, genes), f32),
                pltpu.VMEM((npair, 2 * genes, 128), f32),
                pltpu.VMEM((npair, 2 * genes, 128), f32),
                pltpu.VMEM((nleft, npair, 2 * genes, genes), f32),
                pltpu.VMEM((nleft, npower, 8, genes), f32),
                pltpu.VMEM((nleft, height, genes), f32),
                pltpu.VMEM((2 * npair, height, genes), f32),
                dma((3,)),
                dma((nh - 1,)),
                dma((nh, n0 - 1)),
                dma((nl - 1,)),
                dma((nl, n1 - 1)),
                dma((nl, n1)),
                dma((1,)),
                dma((nh - 1, CHUNKS)),
                dma((nh, n0 - 1)),
                dma((nl - 1, CHUNKS)),
                dma((nl, n1 - 1, CHUNKS)),
                dma((nl, n1, 2)),
                dma((nleft + 2 * npair - 2,)),
                dma((2,)),
                dma((2,)),
            ],
            compiler_params=pltpu.CompilerParams(
                collective_id=0, has_side_effects=True, vmem_limit_bytes=67043328
            ),
        )(powers, expression)
        log_degree, freq, slope, mean_log = pl.pallas_call(
            functools.partial(unpack_kernel, npower),
            out_shape=(
                jax.ShapeDtypeStruct((npower, genes), f32),
                jax.ShapeDtypeStruct((npower, BINS), f32),
                jax.ShapeDtypeStruct((1, npower), f32),
                jax.ShapeDtypeStruct((1, npower), f32),
            ),
            in_specs=[vmem, vmem],
            out_specs=(vmem,) * 4,
        )(log_degree, packed)
        return log_degree, freq, slope.reshape(npower), mean_log.reshape(npower)

    return jax.shard_map(
        on_device,
        mesh=mesh,
        in_specs=(P(("row", "col"), None), P()),
        out_specs=(P(None, ("row", "col")), P(), P(), P()),
        check_vma=False,
    )
```

```python
import functools
import math

import jax
import jax.numpy as jnp
from jax import lax
from jax.experimental import pallas as pl
from jax.experimental.pallas import tpu as pltpu
from jax.sharding import PartitionSpec as P

BINS = 10
EDGES = (0, 2, 4, 6, 7, 8)
CHUNKS = len(EDGES) - 1
LATE = 2
STATS = CHUNKS
STRIP = 32
LOG2E = math.log2(math.e)
LOG10E = math.log10(math.e)
MESH = pl.DeviceIdType.MESH


def split(size):
    low = max(f for f in range(1, math.isqrt(size) + 1) if size % f == 0)
    return size // low, low


def kernel(
    n0, n1, nh, nl, npower, powers_hbm, expr_hbm, log_degree_ref, fit_ref,
    powers_ref, left, right, stats, right_mean, right_inv, raw_ref, sums_ref, partial, degrees,
    load_sem, send_sem,
    far_recv, side_recv, near_recv, up_recv, twin_recv, stat_recv, part_sem, deg_sem,
):
    r, c = lax.axis_index("row"), lax.axis_index("col")
    q, core = r // 2, r % 2
    q1, q0 = q // n0, q % n0
    ch, cl = c // nl, c % nl
    nleft, npair = nh * n0, nl * n1
    _, genes, samples = left.shape
    edges = [genes * e // EDGES[-1] for e in EDGES]
    late = 2 * edges[LATE]

    def device(d0=0, dh=0, d1=0, dl=0, other=False):
        row = (((q1 + d1) % n1) * n0 + (q0 + d0) % n0) * 2 + (1 - core if other else core)
        return row, ((ch + dh) % nh) * nl + (cl + dl) % nl

    def left_slot(dh, d0):
        return ((ch + nh - dh) % nh) * n0 + (q0 + n0 - d0) % n0

    def pair_slot(dl, d1):
        return ((cl + nl - dl) % nl) * n1 + (q1 + n1 - d1) % n1

    own_left, own_pair = left_slot(0, 0), pair_slot(0, 0)
    block = left.at[own_left]

    def left_piece(slot, k):
        if k == STATS:
            return stats.at[slot]
        return left.at[slot, pl.ds(edges[k], edges[k + 1] - edges[k])]

    def right_piece(slot, side, k):
        if k == STATS:
            return stats.at[nleft + slot * 2 + side]
        size = edges[k + 1] - edges[k]
        return right.at[slot, pl.ds(2 * edges[k] + side * size, size)]

    loads = [
        pltpu.make_async_copy(expr_hbm, block, load_sem.at[0]),
        pltpu.make_async_copy(powers_hbm, powers_ref, load_sem.at[1]),
    ]
    for load in loads:
        load.start()
    for k in range(CHUNKS):
        source = expr_hbm.at[pl.ds(edges[k], edges[k + 1] - edges[k])]
        pltpu.make_async_copy(source, right_piece(own_pair, core, k), load_sem.at[2]).start()

    barrier = pltpu.get_barrier_semaphore()
    greeted = [dict(other=True)]
    greeted += [dict(d0=d) for d in range(1, n0)]
    greeted += [dict(d1=d) for d in range(1, n1)]
    greeted += [dict(dh=d) for d in range(1, nh)]
    greeted += [dict(dl=d) for d in range(1, nl)]
    for where in greeted:
        pl.semaphore_signal(barrier, inc=1, device_id=device(**where), device_id_type=MESH)

    loads.append(pltpu.make_async_copy(expr_hbm, block, load_sem.at[2]))
    for load in loads:
        load.wait()

    values = left[own_left].astype(jnp.float32)
    mean = jnp.mean(values, axis=1, keepdims=True)
    centred = values - mean
    inv = lax.rsqrt(jnp.mean(centred * centred, axis=1, keepdims=True) + 1e-06)
    own_stats = jnp.concatenate(
        [jnp.broadcast_to(mean, (genes, 128)).T[0:1, :], jnp.broadcast_to(inv, (genes, 128)).T[0:1, :]], axis=0
    )
    stats[own_left] = own_stats
    stats[nleft + own_pair * 2 + core] = own_stats
    for slot in range(nleft):
        for p in range(npower):
            sums_ref[slot, p] = jnp.zeros((8, genes), jnp.float32)
    exponents = [powers_ref[p].astype(jnp.float32) * LOG2E for p in range(npower)]

    pl.semaphore_wait(barrier, len(greeted))

    def remote(ref, send, recv, where):
        return pltpu.make_async_remote_copy(
            src_ref=ref, dst_ref=ref, send_sem=send, recv_sem=recv, device_id=device(**where), device_id_type=MESH
        )

    flows = [("far", dh, 0) for dh in range(1, nh)] + [("near", dl, 0) for dl in range(1, nl)]
    flows += [("side", dh, d0) for dh in range(nh) for d0 in range(1, n0)]
    flows += [("up", dl, d1) for dl in range(nl) for d1 in range(1, n1)]
    flows += [("twin", dl, d1) for dl in range(nl) for d1 in range(n1)]

    def sems(kind, a, b, k):
        if k == STATS:
            return send_sem.at[0], stat_recv.at[flows.index((kind, a, b))]
        if kind == "far":
            return send_sem.at[1], far_recv.at[a - 1, k]
        if kind == "near":
            return send_sem.at[1], near_recv.at[a - 1, k]
        if kind == "side":
            return send_sem.at[1], side_recv.at[a, b - 1]
        if kind == "up":
            return send_sem.at[2], up_recv.at[a, b - 1, k]
        return send_sem.at[2], twin_recv.at[a, b, int(k >= LATE)]

    def send(kind, a, b, k):
        if kind == "far":
            ref, where = left_piece(own_left, k), dict(dh=a)
        elif kind == "side":
            ref, where = left_piece(left_slot(a, 0), k), dict(d0=b)
        elif kind == "near":
            ref, where = right_piece(own_pair, core, k), dict(dl=a)
        elif kind == "up":
            ref, where = right_piece(pair_slot(a, 0), core, k), dict(d1=b)
        else:
            ref, where = right_piece(pair_slot(a, b), core, k), dict(other=True)
        remote(ref, *sems(kind, a, b, k), where).start()

    def wait(kind, a, b, k, ref):
        remote(ref, *sems(kind, a, b, k), dict(other=True)).wait_recv()

    def wait_far(dh, k):
        wait("far", dh, 0, k, left_piece(left_slot(dh, 0), k))

    def wait_side(dh, d0, k):
        wait("side", dh, d0, k, left_piece(left_slot(dh, d0), k) if k == STATS else left.at[left_slot(dh, d0)])

    def wait_near(dl, k):
        wait("near", dl, 0, k, right_piece(pair_slot(dl, 0), core, k))

    def wait_up(dl, d1, k):
        wait("up", dl, d1, k, right_piece(pair_slot(dl, d1), core, k))

    def wait_twin(dl, d1, k):
        slot = pair_slot(dl, d1)
        if k == STATS:
            ref = right_piece(slot, 1 - core, k)
        else:
            ref = right.at[slot, pl.ds(0, edges[LATE]) if k < LATE else pl.ds(late, genes - edges[LATE])]
        wait("twin", dl, d1, k, ref)

    for k in (STATS, *range(CHUNKS)):
        for first in (0, 1):
            @pl.when(core == first)
            def _():
                for kind in ("far", "near") if first == 0 else ("near", "far"):
                    for a in range(1, nh if kind == "far" else nl):
                        send(kind, a, 0, k)

        for d0 in range(1, n0):
            send("side", 0, d0, k)
        for d1 in range(1, n1):
            send("up", 0, d1, k)
        send("twin", 0, 0, k)

    def multiply(ls, blocks, ps, pairs, lo=0, hi=2 * genes):
        size = hi - lo
        lhs = right[pl.ds(ps, pairs), lo:hi].reshape(pairs * size, samples)
        rhs = left[pl.ds(ls, blocks)].reshape(blocks * genes, samples)
        raw = lax.dot_general(lhs, rhs, (((1,), (1,)), ((), ())), preferred_element_type=jnp.float32)
        for a in range(blocks):
            for b in range(pairs):
                raw_ref[ls + a, ps + b, lo:hi] = raw[b * size:(b + 1) * size, a * genes:(a + 1) * genes]

    def accumulate(ls, ps, lo=0, hi=2 * genes):
        mean_row, inv_row = stats[ls, 0:1, :], stats[ls, 1:2, :]
        totals = [None] * npower
        for s in range(lo, hi, STRIP):
            raw = raw_ref[ls, ps, s:s + STRIP, :]
            mean_col, inv_col = right_mean[ps, s:s + STRIP, :], right_inv[ps, s:s + STRIP, :]
            pearson = (raw * (1.0 / samples) - mean_col * mean_row) * inv_col * inv_row
            log_abs = jnp.log(jnp.abs(pearson))
            for p in range(npower):
                part = jnp.sum(jnp.exp2(exponents[p] * log_abs).reshape(STRIP // 8, 8, genes), axis=0)
                totals[p] = part if totals[p] is None else totals[p] + part
        for p in range(npower):
            sums_ref[ls, p] = sums_ref[ls, p] + totals[p]

    def part(ls, blocks, ps, pairs, lo=0, hi=2 * genes):
        return ls, blocks, ps, pairs, lo, hi

    def run(*parts):
        for each in parts:
            multiply(*each)
        for each in parts:
            add(*each)

    def add(ls, blocks, ps, pairs, lo=0, hi=2 * genes):
        def body(u, _):
            accumulate(ls + lax.rem(u, blocks), ps + lax.div(u, blocks), lo, hi)
            return 0

        lax.fori_loop(0, blocks * pairs, body, 0)

    def columns(dl, d1):
        slot = pair_slot(dl, d1)
        for side in (0, 1):
            row = stats[nleft + slot * 2 + side]
            mean_col = jnp.broadcast_to(row[0:1], (128, genes)).T
            inv_col = jnp.broadcast_to(row[1:2], (128, genes)).T
            for k in range(CHUNKS):
                low, high = edges[k], edges[k + 1]
                window = pl.ds(2 * low + side * (high - low), high - low)
                right_mean[slot, window] = mean_col[low:high]
                right_inv[slot, window] = inv_col[low:high]

    own_row, own_line = ch * n0, cl * n1
    far_pairs = [(dl, 0) for dl in range(1, nl)]
    rest_pairs = [(dl, d1) for dl in range(1, nl) for d1 in range(1, n1)]
    far_rows = [(ch + nh - dh) % nh * n0 for dh in range(1, nh)]
    far_blocks = [left_slot(dh, 0) for dh in range(1, nh)]
    rest_blocks = [(dh, d0) for dh in range(1, nh) for d0 in range(1, n0)]

    early_blocks = [(0, d0) for d0 in range(n0)]
    late_blocks = [(dh, d0) for dh in range(1, nh) for d0 in range(n0)]
    far_lines = [(cl + nl - dl) % nl * n1 for dl in range(1, nl)]

    def index_of(a, b, dh, d0):
        return (a * n0 + b) * nleft + dh * n0 + d0

    def send_partials(group):
        for m in group:
            slot = left_slot(*m)
            rows = [jnp.sum(sums_ref[slot, p], axis=0, keepdims=True) for p in range(npower)]
            partial[index_of(0, 0, *m)] = jnp.concatenate(rows, axis=0)
        for a in reversed(range(nh)):
            for b in reversed(range(n0)):
                for m in group:
                    if a or b:
                        pltpu.make_async_remote_copy(
                            src_ref=partial.at[index_of(0, 0, *m)], dst_ref=partial.at[index_of(a, b, *m)],
                            send_sem=part_sem.at[0], recv_sem=part_sem.at[1 if group is early_blocks else 2],
                            device_id=device(dh=a, d0=b), device_id_type=MESH,
                        ).start()

    def pass_up(k):
        for d1 in range(1, n1):
            wait_up(0, d1, k)
            send("twin", 0, d1, k)

    def pass_far(k):
        for dl in range(1, nl):
            wait_near(dl, k)
            for d1 in range(1, n1):
                send("up", dl, d1, k)
            send("twin", dl, 0, k)
        for dh in range(1, nh):
            wait_far(dh, k)
            for d0 in range(1, n0):
                send("side", dh, d0, k)

    def pass_rest(k):
        for dl, d1 in rest_pairs:
            wait_up(dl, d1, k)
            send("twin", dl, d1, k)

    wait_twin(0, 0, STATS)
    wait_twin(0, 0, 0)
    wait_twin(0, 0, LATE)
    columns(0, 0)
    pass_up(STATS)
    pass_far(STATS)
    pass_up(0)
    pass_up(1)
    pass_far(0)
    pass_rest(STATS)
    pass_up(2)
    pass_up(3)
    for dl in range(nl):
        for d1 in range(n1):
            if dl or d1:
                wait_twin(dl, d1, STATS)
                columns(dl, d1)
    for dh in range(nh):
        for d0 in range(1, n0):
            wait_side(dh, d0, STATS)
    pass_up(4)
    pass_far(1)
    for d0 in range(1, n0):
        wait_side(0, d0, 0)
    run(part(own_row, n0, own_pair, 1))
    pass_rest(0)
    for d1 in range(1, n1):
        wait_twin(0, d1, 0)
        wait_twin(0, d1, LATE)
        run(part(own_row, n0, pair_slot(0, d1), 1))
    pass_far(2)
    for m in far_pairs:
        wait_twin(*m, 0)
    run(*[part(own_row, n0, pair_slot(*m), 1, 0, late) for m in far_pairs])
    pass_rest(1)
    pass_far(3)
    pass_far(4)
    run(*[part(b, 1, own_line, n1) for b in far_blocks])
    for m in far_pairs:
        wait_twin(*m, LATE)
    for m in rest_pairs:
        wait_twin(*m, 0)
    run(
        *[part(b, 1, pair_slot(*m), 1) for b in far_blocks for m in far_pairs],
        *[part(own_row, n0, pair_slot(*m), 1, late) for m in far_pairs],
        *[part(own_row, n0, pair_slot(*m), 1, 0, late) for m in rest_pairs],
        *[part(b, 1, pair_slot(*m), 1, 0, late) for b in far_blocks for m in rest_pairs],
    )
    for k in range(2, CHUNKS):
        pass_rest(k)
    for m in rest_blocks:
        wait_side(*m, 0)
    run(
        *[part(left_slot(*b), 1, own_line, n1) for b in rest_blocks],
        *[part(left_slot(*b), 1, pair_slot(*m), 1) for b in rest_blocks for m in far_pairs],
        *[part(left_slot(*b), 1, pair_slot(*m), 1, 0, late) for b in rest_blocks for m in rest_pairs],
    )
    for m in rest_pairs:
        wait_twin(*m, LATE)
    for m in rest_pairs:
        multiply(0, nleft, pair_slot(*m), 1, late)
    for m in rest_pairs:
        add(own_row, n0, pair_slot(*m), 1, late)
    send_partials(early_blocks)
    for m in rest_pairs:
        for b in far_rows:
            add(b, n0, pair_slot(*m), 1, late)

    send_partials(late_blocks)
    for group, sem in ((early_blocks, 1), (late_blocks, 2)):
        if group:
            count = (nleft - 1) * len(group)
            remote(partial.at[pl.ds(0, count)], part_sem.at[0], part_sem.at[sem], dict(other=True)).wait_recv()
    lines = []
    for dh in range(nh):
        for d0 in range(n0):
            total = partial[index_of(0, 0, dh, d0)]
            for a in range(nh):
                for b in range(n0):
                    if a or b:
                        total = total + partial[index_of(a, b, (dh - a) % nh, (d0 - b) % n0)]
            lines.append(total)
    mine = lines[0]
    height = degrees.shape[1]
    if height > nleft * npower:
        lines.append(jnp.zeros((height - nleft * npower, genes), jnp.float32))
    total = jnp.concatenate(lines, axis=0)
    own = own_pair * 2 + core
    degrees[own] = total

    for dl in reversed(range(nl)):
        for d1 in reversed(range(n1)):
            for o in (True, False):
                if dl or d1 or o:
                    remote(degrees.at[own], deg_sem.at[0], deg_sem.at[1], dict(dl=dl, d1=d1, other=o)).start()
    log_degree_ref[...] = jnp.log(mine) * LOG10E

    pair_flows = [flow for flow in flows if flow[0] in ("up", "twin")]
    pairs_ref = right.reshape(2 * npair, genes, samples)
    for group in ([flow for flow in flows if flow not in pair_flows], pair_flows):
        remote(pairs_ref.at[pl.ds(0, len(group))], *sems(*group[0], 0), dict(other=True)).wait_send()
    remote(stats.at[pl.ds(0, len(flows))], *sems(*flows[0], STATS), dict(other=True)).wait_send()
    others = partial.at[pl.ds(0, (nleft - 1) * nleft)]
    remote(others, part_sem.at[0], part_sem.at[1], dict(other=True)).wait_send()
    rest = degrees.at[pl.ds(0, 2 * npair - 1)]
    remote(rest, deg_sem.at[0], deg_sem.at[1], dict(other=True)).wait_recv()
    fit(genes * nleft * npair * 2, nleft, npower, degrees, fit_ref)
    remote(rest, deg_sem.at[0], deg_sem.at[1], dict(other=True)).wait_send()


def fit(genes_all, nleft, npower, degrees, fit_ref):
    blocks, height, genes = degrees.shape
    padded = npower + 8 - npower % 8
    spare = height - nleft * npower

    def fold(values, combine):
        total = values[:npower]
        for block in range(1, nleft):
            total = combine(total, values[block * npower:(block + 1) * npower])
        return jnp.concatenate([total, jnp.ones((padded - npower, 1), jnp.float32)], axis=0)

    best = lax.fori_loop(1, blocks, lambda index, best: jnp.maximum(best, degrees[index]), degrees[0])
    peak = fold(jnp.max(best, axis=1, keepdims=True), jnp.maximum)
    scales = [(BINS / peak)[:npower]] * nleft
    if spare:
        scales.append(jnp.ones((spare, 1), jnp.float32))
    scale = jnp.broadcast_to(jnp.concatenate(scales, axis=0), (height, genes))

    def weigh(index, carry):
        carry = list(carry)
        degree = degrees[index]
        position = jnp.clip(degree * scale - 0.5, 0.0, BINS - 1.0)
        for b in range(BINS):
            carry[b] = carry[b] + jnp.maximum(0.0, 1.0 - jnp.abs(position - b))
        carry[BINS] = carry[BINS] + degree
        return tuple(carry)

    totals = lax.fori_loop(0, blocks, weigh, tuple(jnp.zeros((height, genes), jnp.float32) for _ in range(BINS + 1)))
    totals = [fold(jnp.sum(total, axis=1, keepdims=True), jnp.add) for total in totals]
    lane = lax.broadcasted_iota(jnp.int32, (padded, 128), 1)
    line = lax.broadcasted_iota(jnp.int32, (padded, 128), 0)
    freq = jnp.zeros((padded, 128), jnp.float32)
    for b in range(BINS):
        freq = jnp.where(lane == b, totals[b], freq)
    freq = freq / genes_all
    fit_ref[0:padded, :] = freq
    mean_log = jnp.log(totals[BINS] / genes_all) * LOG10E
    logs = [math.log10(b + 0.5) for b in range(BINS)]
    deviations = [value - sum(logs) / BINS for value in logs]
    scale = sum(value * value for value in deviations)
    xdev = jnp.zeros((padded, 128), jnp.float32)
    for b in range(BINS):
        xdev = jnp.where(lane == b, deviations[b] / scale, xdev)
    yfit = jnp.log(freq + 1.0 / genes_all) * LOG10E
    slope = jnp.sum(xdev * yfit, axis=1, keepdims=True)
    on_line = jnp.logical_and(lane == line, line < npower)
    fit_ref[padded:padded + 1, :] = jnp.sum(jnp.where(on_line, slope, 0.0), axis=0, keepdims=True)
    fit_ref[padded + 1:padded + 2, :] = jnp.sum(jnp.where(on_line, mean_log, 0.0), axis=0, keepdims=True)


def unpack_kernel(npower, log_degree_in, fit_in, log_degree_ref, freq_ref, slope_ref, mean_log_ref):
    padded = fit_in.shape[0] - 8
    log_degree_ref[...] = log_degree_in[...]
    freq_ref[...] = fit_in[0:npower, :BINS]
    slope_ref[...] = fit_in[padded:padded + 1, :npower]
    mean_log_ref[...] = fit_in[padded + 1:padded + 2, :npower]


def solution(mesh):
    nr, nc = mesh.shape["row"], mesh.shape["col"]
    n1, n0 = split(nr // 2)
    nh, nl = split(nc)

    def on_device(expression, powers):
        genes, samples = expression.shape
        npower = powers.shape[0]
        nleft, npair = nh * n0, nl * n1
        height = -(-npower * nleft // 8) * 8
        vmem = pl.BlockSpec(memory_space=pltpu.VMEM)
        hbm = pl.BlockSpec(memory_space=pltpu.HBM)
        dma = pltpu.SemaphoreType.DMA
        f32 = jnp.float32
        padded = npower + 8 - npower % 8
        log_degree, packed = pl.pallas_call(
            functools.partial(kernel, n0, n1, nh, nl, npower),
            out_shape=(
                pltpu.VMEM((npower, genes), f32),
                pltpu.VMEM((padded + 8, 128), f32),
            ),
            in_specs=[hbm, hbm],
            out_specs=(vmem, vmem),
            scratch_shapes=[
                pltpu.SMEM((npower,), jnp.int32),
                pltpu.VMEM((nleft, genes, samples), jnp.bfloat16),
                pltpu.VMEM((npair, 2 * genes, samples), jnp.bfloat16),
                pltpu.VMEM((nleft + 2 * npair, 2, genes), f32),
                pltpu.VMEM((npair, 2 * genes, 128), f32),
                pltpu.VMEM((npair, 2 * genes, 128), f32),
                pltpu.VMEM((nleft, npair, 2 * genes, genes), f32),
                pltpu.VMEM((nleft, npower, 8, genes), f32),
                pltpu.VMEM((nleft * nleft, npower, genes), f32),
                pltpu.VMEM((2 * npair, height, genes), f32),
                dma((3,)),
                dma((3,)),
                dma((nh - 1, CHUNKS)),
                dma((nh, n0 - 1)),
                dma((nl - 1, CHUNKS)),
                dma((nl, n1 - 1, CHUNKS)),
                dma((nl, n1, 2)),
                dma((nleft + 2 * npair - 2,)),
                dma((3,)),
                dma((2,)),
            ],
            compiler_params=pltpu.CompilerParams(
                collective_id=0, has_side_effects=True, vmem_limit_bytes=67043328 - 128 * 1024
            ),
        )(powers, expression)
        log_degree, freq, slope, mean_log = pl.pallas_call(
            functools.partial(unpack_kernel, npower),
            out_shape=(
                jax.ShapeDtypeStruct((npower, genes), f32),
                jax.ShapeDtypeStruct((npower, BINS), f32),
                jax.ShapeDtypeStruct((1, npower), f32),
                jax.ShapeDtypeStruct((1, npower), f32),
            ),
            in_specs=[vmem, vmem],
            out_specs=(vmem,) * 4,
            compiler_params=pltpu.CompilerParams(vmem_limit_bytes=1 << 20),
        )(log_degree, packed)
        return log_degree, freq, slope.reshape(npower), mean_log.reshape(npower)

    return jax.shard_map(
        on_device,
        mesh=mesh,
        in_specs=(P(("row", "col"), None), P()),
        out_specs=(P(None, ("row", "col")), P(), P(), P()),
        check_vma=False,
    )
```

```python
import functools
import math

import jax
import jax.numpy as jnp
from jax import lax
from jax.experimental import pallas as pl
from jax.experimental.pallas import tpu as pltpu
from jax.sharding import PartitionSpec as P

BINS = 10
EDGES = (0, 2, 4, 6, 7, 8)
CHUNKS = len(EDGES) - 1
LATE = 2
STATS = CHUNKS
STRIP = 32
UNROLL = 2
LOG2E = math.log2(math.e)
LOG10E = math.log10(math.e)
MESH = pl.DeviceIdType.MESH


def split(size):
    low = max(f for f in range(1, math.isqrt(size) + 1) if size % f == 0)
    return size // low, low


def kernel(
    n0, n1, nh, nl, npower, powers_hbm, expr_hbm, log_degree_ref, fit_ref,
    powers_ref, left, right, stats, right_mean, right_inv, raw_ref, sums_ref, partial, degrees,
    load_sem, send_sem,
    far_recv, side_recv, near_recv, up_recv, twin_recv, stat_recv, part_sem, deg_sem,
):
    r, c = lax.axis_index("row"), lax.axis_index("col")
    q, core = r // 2, r % 2
    q1, q0 = q // n0, q % n0
    ch, cl = c // nl, c % nl
    nleft, npair = nh * n0, nl * n1
    _, genes, samples = left.shape
    edges = [genes * e // EDGES[-1] for e in EDGES]
    late = 2 * edges[LATE]

    def device(d0=0, dh=0, d1=0, dl=0, other=False):
        row = (((q1 + d1) % n1) * n0 + (q0 + d0) % n0) * 2 + (1 - core if other else core)
        return row, ((ch + dh) % nh) * nl + (cl + dl) % nl

    def left_slot(dh, d0):
        return ((ch + nh - dh) % nh) * n0 + (q0 + n0 - d0) % n0

    def pair_slot(dl, d1):
        return ((cl + nl - dl) % nl) * n1 + (q1 + n1 - d1) % n1

    own_left, own_pair = left_slot(0, 0), pair_slot(0, 0)
    block = left.at[own_left]

    def left_piece(slot, k):
        if k == STATS:
            return stats.at[slot]
        return left.at[slot, pl.ds(edges[k], edges[k + 1] - edges[k])]

    def right_piece(slot, side, k):
        if k == STATS:
            return stats.at[nleft + slot * 2 + side]
        size = edges[k + 1] - edges[k]
        return right.at[slot, pl.ds(2 * edges[k] + side * size, size)]

    for k in range(CHUNKS):
        source = expr_hbm.at[pl.ds(edges[k], edges[k + 1] - edges[k])]
        pltpu.make_async_copy(source, right_piece(own_pair, core, k), load_sem.at[0 if k == 0 else 1]).start()
    loads = [
        pltpu.make_async_copy(expr_hbm, block, load_sem.at[2]),
        pltpu.make_async_copy(powers_hbm, powers_ref, load_sem.at[3]),
    ]
    for load in loads:
        load.start()

    barrier = pltpu.get_barrier_semaphore()
    greeted = [dict(other=True)]
    greeted += [dict(d0=d) for d in range(1, n0)]
    greeted += [dict(d1=d) for d in range(1, n1)]
    greeted += [dict(dh=d) for d in range(1, nh)]
    greeted += [dict(dl=d) for d in range(1, nl)]
    for where in greeted:
        pl.semaphore_signal(barrier, inc=1, device_id=device(**where), device_id_type=MESH)

    def load_wait(low, high, sem):
        window = pl.ds(edges[low], edges[high] - edges[low])
        pltpu.make_async_copy(expr_hbm.at[window], left.at[own_left, window], load_sem.at[sem]).wait()

    load_wait(0, 1, 0)
    pl.semaphore_wait(barrier, len(greeted))

    def remote(ref, send, recv, where, src=None):
        return pltpu.make_async_remote_copy(
            src_ref=ref if src is None else src, dst_ref=ref, send_sem=send, recv_sem=recv, device_id=device(**where), device_id_type=MESH
        )

    flows = [("far", dh, 0) for dh in range(1, nh)] + [("near", dl, 0) for dl in range(1, nl)]
    flows += [("side", dh, d0) for dh in range(nh) for d0 in range(1, n0)]
    flows += [("up", dl, d1) for dl in range(nl) for d1 in range(1, n1)]
    flows += [("twin", dl, d1) for dl in range(nl) for d1 in range(n1)]

    def sems(kind, a, b, k):
        if k == STATS:
            return send_sem.at[0], stat_recv.at[flows.index((kind, a, b))]
        if kind == "far":
            return send_sem.at[1], far_recv.at[a - 1, k]
        if kind == "near":
            return send_sem.at[1], near_recv.at[a - 1, k]
        if kind == "side":
            return send_sem.at[1], side_recv.at[a, b - 1]
        if kind == "up":
            return send_sem.at[2], up_recv.at[a, b - 1, k]
        return send_sem.at[2], twin_recv.at[a, b, int(k >= LATE)]

    def send(kind, a, b, k):
        if kind == "far":
            ref, where = left_piece(own_left, k), dict(dh=a)
        elif kind == "side":
            ref, where = left_piece(left_slot(a, 0), k), dict(d0=b)
        elif kind == "near":
            ref, where = right_piece(own_pair, core, k), dict(dl=a)
        elif kind == "up":
            ref, where = right_piece(pair_slot(a, 0), core, k), dict(d1=b)
        else:
            ref, where = right_piece(pair_slot(a, b), core, k), dict(other=True)
        own = right_piece(own_pair, core, k) if kind == "far" or (kind == "side" and a == 0) else None
        remote(ref, *sems(kind, a, b, k), where, own).start()

    def wait(kind, a, b, k, ref):
        remote(ref, *sems(kind, a, b, k), dict(other=True)).wait_recv()

    def wait_far(dh, k):
        wait("far", dh, 0, k, left_piece(left_slot(dh, 0), k))

    def wait_side(dh, d0, k):
        wait("side", dh, d0, k, left_piece(left_slot(dh, d0), k) if k == STATS else left.at[left_slot(dh, d0)])

    def wait_near(dl, k):
        wait("near", dl, 0, k, right_piece(pair_slot(dl, 0), core, k))

    def wait_up(dl, d1, k):
        wait("up", dl, d1, k, right_piece(pair_slot(dl, d1), core, k))

    def wait_twin(dl, d1, k):
        slot = pair_slot(dl, d1)
        if k == STATS:
            ref = right_piece(slot, 1 - core, k)
        else:
            ref = right.at[slot, pl.ds(0, edges[LATE]) if k < LATE else pl.ds(late, genes - edges[LATE])]
        wait("twin", dl, d1, k, ref)

    def send_own(k):
        for first in (0, 1):
            @pl.when(core == first)
            def _():
                for kind in ("far", "near") if first == 0 else ("near", "far"):
                    for a in range(1, nh if kind == "far" else nl):
                        send(kind, a, 0, k)

        for d0 in range(1, n0):
            send("side", 0, d0, k)
        for d1 in range(1, n1):
            send("up", 0, d1, k)
        send("twin", 0, 0, k)

    send_own(0)
    load_wait(1, CHUNKS, 1)
    for load in loads:
        load.wait()
    values = left[own_left].astype(jnp.float32)
    mean = jnp.mean(values, axis=1, keepdims=True)
    centred = values - mean
    inv = lax.rsqrt(jnp.mean(centred * centred, axis=1, keepdims=True) + 1e-06)
    own_stats = jnp.concatenate(
        [jnp.broadcast_to(mean, (genes, 128)).T[0:1, :], jnp.broadcast_to(inv, (genes, 128)).T[0:1, :]], axis=0
    )
    stats[own_left] = own_stats
    stats[nleft + own_pair * 2 + core] = own_stats
    for k in (STATS, *range(1, CHUNKS)):
        send_own(k)
    for slot in range(nleft):
        for p in range(npower):
            sums_ref[slot, p] = jnp.zeros((8, genes), jnp.float32)
    exponents = [powers_ref[p].astype(jnp.float32) * LOG2E for p in range(npower)]

    def multiply(ls, blocks, ps, pairs, lo=0, hi=2 * genes):
        size = hi - lo
        lhs = right[pl.ds(ps, pairs), lo:hi].reshape(pairs * size, samples)
        rhs = left[pl.ds(ls, blocks)].reshape(blocks * genes, samples)
        raw = lax.dot_general(lhs, rhs, (((1,), (1,)), ((), ())), preferred_element_type=jnp.float32)
        for a in range(blocks):
            for b in range(pairs):
                raw_ref[ls + a, ps + b, lo:hi] = raw[b * size:(b + 1) * size, a * genes:(a + 1) * genes]

    def accumulate(ls, ps, lo=0, hi=2 * genes):
        mean_row, inv_row = stats[ls, 0:1, :], stats[ls, 1:2, :]
        totals = [None] * npower
        for s in range(lo, hi, STRIP):
            raw = raw_ref[ls, ps, s:s + STRIP, :]
            mean_col, inv_col = right_mean[ps, s:s + STRIP, :], right_inv[ps, s:s + STRIP, :]
            pearson = (raw * (1.0 / samples) - mean_col * mean_row) * inv_col * inv_row
            log_abs = jnp.log(jnp.abs(pearson))
            for p in range(npower):
                part = jnp.sum(jnp.exp2(exponents[p] * log_abs).reshape(STRIP // 8, 8, genes), axis=0)
                totals[p] = part if totals[p] is None else totals[p] + part
        for p in range(npower):
            sums_ref[ls, p] = sums_ref[ls, p] + totals[p]

    def part(ls, blocks, ps, pairs, lo=0, hi=2 * genes):
        return ls, blocks, ps, pairs, lo, hi

    def run(*parts):
        multiply(*parts[0])
        for each, later in zip(parts, parts[1:] + (None,)):
            if later is not None:
                multiply(*later)
            add(*each)

    def add(ls, blocks, ps, pairs, lo=0, hi=2 * genes):
        def body(u, _):
            accumulate(ls + lax.rem(u, blocks), ps + lax.div(u, blocks), lo, hi)
            return 0

        if blocks * pairs <= 4:
            for u in range(blocks * pairs):
                accumulate(ls + u % blocks, ps + u // blocks, lo, hi)
        else:
            lax.fori_loop(0, blocks * pairs, body, 0, unroll=UNROLL)

    def columns(dl, d1):
        slot = pair_slot(dl, d1)
        for side in (0, 1):
            row = stats[nleft + slot * 2 + side]
            mean_col = jnp.broadcast_to(row[0:1], (128, genes)).T
            inv_col = jnp.broadcast_to(row[1:2], (128, genes)).T
            for k in range(CHUNKS):
                low, high = edges[k], edges[k + 1]
                window = pl.ds(2 * low + side * (high - low), high - low)
                right_mean[slot, window] = mean_col[low:high]
                right_inv[slot, window] = inv_col[low:high]

    own_row, own_line = ch * n0, cl * n1
    far_pairs = [(dl, 0) for dl in range(1, nl)]
    rest_pairs = [(dl, d1) for dl in range(1, nl) for d1 in range(1, n1)]
    far_rows = [(ch + nh - dh) % nh * n0 for dh in range(1, nh)]
    far_blocks = [left_slot(dh, 0) for dh in range(1, nh)]
    rest_blocks = [(dh, d0) for dh in range(1, nh) for d0 in range(1, n0)]

    early_blocks = [(0, d0) for d0 in range(n0)]
    late_blocks = [(dh, d0) for dh in range(1, nh) for d0 in range(n0)]
    far_lines = [(cl + nl - dl) % nl * n1 for dl in range(1, nl)]

    def index_of(a, b, dh, d0):
        return (a * n0 + b) * nleft + dh * n0 + d0

    def send_partials(group):
        for m in group:
            slot = left_slot(*m)
            rows = [jnp.sum(sums_ref[slot, p], axis=0, keepdims=True) for p in range(npower)]
            partial[index_of(0, 0, *m)] = jnp.concatenate(rows, axis=0)
        first, count = index_of(0, 0, *group[0]), len(group)
        for a in reversed(range(nh)):
            for b in reversed(range(n0)):
                if a or b:
                    pltpu.make_async_remote_copy(
                        src_ref=partial.at[pl.ds(first, count)],
                        dst_ref=partial.at[pl.ds(index_of(a, b, *group[0]), count)],
                        send_sem=part_sem.at[0], recv_sem=part_sem.at[1 if group is early_blocks else 2],
                        device_id=device(dh=a, d0=b), device_id_type=MESH,
                    ).start()

    def pass_up(k):
        for d1 in range(1, n1):
            wait_up(0, d1, k)
            send("twin", 0, d1, k)

    def pass_far(k):
        for dl in range(1, nl):
            wait_near(dl, k)
            for d1 in range(1, n1):
                send("up", dl, d1, k)
            send("twin", dl, 0, k)
        for dh in range(1, nh):
            wait_far(dh, k)
            for d0 in range(1, n0):
                send("side", dh, d0, k)

    def pass_rest(k):
        for dl, d1 in rest_pairs:
            wait_up(dl, d1, k)
            send("twin", dl, d1, k)

    wait_twin(0, 0, STATS)
    wait_twin(0, 0, 0)
    wait_twin(0, 0, LATE)
    columns(0, 0)
    pass_up(0)
    pass_up(STATS)
    pass_up(1)
    pass_far(0)
    pass_far(STATS)
    for k in range(2, CHUNKS):
        pass_up(k)
    for d1 in range(1, n1):
        wait_twin(0, d1, STATS)
        columns(0, d1)
    for d0 in range(1, n0):
        wait_side(0, d0, STATS)
        wait_side(0, d0, 0)
    pass_far(1)
    run(part(own_row, n0, own_pair, 1))
    for d1 in range(1, n1):
        wait_twin(0, d1, 0)
        wait_twin(0, d1, LATE)
        run(part(own_row, n0, pair_slot(0, d1), 1))
    pass_rest(STATS)
    pass_rest(0)
    pass_far(2)
    for m in far_pairs:
        wait_twin(*m, STATS)
        columns(*m)
        wait_twin(*m, 0)
    run(*[part(own_row, n0, pair_slot(*m), 1, 0, late) for m in far_pairs])
    for m in rest_pairs:
        wait_twin(*m, STATS)
        columns(*m)
    for dh in range(1, nh):
        for d0 in range(1, n0):
            wait_side(dh, d0, STATS)
    pass_rest(1)
    pass_far(3)
    for k in range(4, CHUNKS):
        pass_far(k)
    run(*[part(b, 1, own_line, n1) for b in far_blocks])
    for m in far_pairs:
        wait_twin(*m, LATE)
    for m in rest_pairs:
        wait_twin(*m, 0)
    run(
        *[part(b, 1, pair_slot(*m), 1) for b in far_blocks for m in far_pairs],
        *[part(own_row, n0, pair_slot(*m), 1, late) for m in far_pairs],
        *[part(own_row, n0, pair_slot(*m), 1, 0, late) for m in rest_pairs],
        *[part(b, 1, pair_slot(*m), 1, 0, late) for b in far_blocks for m in rest_pairs],
    )
    for k in range(2, CHUNKS):
        pass_rest(k)
    for m in rest_blocks:
        wait_side(*m, 0)
    run(
        *[part(left_slot(*b), 1, own_line, n1) for b in rest_blocks],
        *[part(left_slot(*b), 1, pair_slot(*m), 1) for b in rest_blocks for m in far_pairs],
        *[part(left_slot(*b), 1, pair_slot(*m), 1, 0, late) for b in rest_blocks for m in rest_pairs],
    )
    for m in rest_pairs:
        wait_twin(*m, LATE)
    for m in rest_pairs:
        multiply(0, nleft, pair_slot(*m), 1, late)
    for m in rest_pairs:
        add(own_row, n0, pair_slot(*m), 1, late)
    send_partials(early_blocks)
    for m in rest_pairs:
        for b in far_rows:
            add(b, n0, pair_slot(*m), 1, late)

    send_partials(late_blocks)
    for group, sem in ((early_blocks, 1), (late_blocks, 2)):
        if group:
            count = (nleft - 1) * len(group)
            remote(partial.at[pl.ds(0, count)], part_sem.at[0], part_sem.at[sem], dict(other=True)).wait_recv()
    lines = []
    for dh in range(nh):
        for d0 in range(n0):
            total = partial[index_of(0, 0, dh, d0)]
            for a in range(nh):
                for b in range(n0):
                    if a or b:
                        total = total + partial[index_of(a, b, (dh - a) % nh, (d0 - b) % n0)]
            lines.append(total)
    mine = lines[0]
    height = degrees.shape[1]
    if height > nleft * npower:
        lines.append(jnp.zeros((height - nleft * npower, genes), jnp.float32))
    total = jnp.concatenate(lines, axis=0)
    own = own_pair * 2 + core
    degrees[own] = total

    for dl in reversed(range(nl)):
        for d1 in reversed(range(n1)):
            for o in (True, False):
                if dl or d1 or o:
                    remote(degrees.at[own], deg_sem.at[0], deg_sem.at[1], dict(dl=dl, d1=d1, other=o)).start()
    log_degree_ref[...] = jnp.log(mine) * LOG10E

    pair_flows = [flow for flow in flows if flow[0] in ("up", "twin")]
    pairs_ref = right.reshape(2 * npair, genes, samples)
    for group in ([flow for flow in flows if flow not in pair_flows], pair_flows):
        remote(pairs_ref.at[pl.ds(0, len(group))], *sems(*group[0], 0), dict(other=True)).wait_send()
    remote(stats.at[pl.ds(0, len(flows))], *sems(*flows[0], STATS), dict(other=True)).wait_send()
    others = partial.at[pl.ds(0, (nleft - 1) * nleft)]
    remote(others, part_sem.at[0], part_sem.at[1], dict(other=True)).wait_send()
    rest = degrees.at[pl.ds(0, 2 * npair - 1)]
    remote(rest, deg_sem.at[0], deg_sem.at[1], dict(other=True)).wait_recv()
    fit(genes * nleft * npair * 2, nleft, npower, degrees, fit_ref)
    remote(rest, deg_sem.at[0], deg_sem.at[1], dict(other=True)).wait_send()


def fit(genes_all, nleft, npower, degrees, fit_ref):
    blocks, height, genes = degrees.shape
    padded = fit_ref.shape[0] - 8

    def fold(values, combine):
        total = values[:npower]
        for block in range(1, nleft):
            total = combine(total, values[block * npower:(block + 1) * npower])
        return total

    best = degrees[0]
    for index in range(1, blocks):
        best = jnp.maximum(best, degrees[index])
    best = jnp.broadcast_to(jnp.max(best, axis=1, keepdims=True), (height, genes))
    scales = [BINS / fold(best, jnp.maximum)] * nleft
    if height > nleft * npower:
        scales.append(jnp.ones((height - nleft * npower, genes), jnp.float32))
    scale = jnp.concatenate(scales, axis=0)
    positions = [jnp.clip(degrees[index] * scale - 0.5, 0.0, BINS - 1.0) for index in range(blocks)]
    lane = lax.broadcasted_iota(jnp.int32, (height, 128), 1)
    table = jnp.zeros((height, 128), jnp.float32)
    for b in range(BINS + 1):
        total = None
        for index in range(blocks):
            term = degrees[index] if b == BINS else jnp.maximum(0.0, 1.0 - jnp.abs(positions[index] - b))
            total = term if total is None else total + term
        table = jnp.where(lane == b, jnp.sum(total, axis=1, keepdims=True), table)
    table = fold(table, jnp.add) / genes_all
    fit_ref[0:npower, :] = table
    lane = lax.broadcasted_iota(jnp.int32, (npower, 128), 1)
    line = lax.broadcasted_iota(jnp.int32, (npower, 128), 0)
    logs = [math.log10(b + 0.5) for b in range(BINS)]
    deviations = [value - sum(logs) / BINS for value in logs]
    square = sum(value * value for value in deviations)
    xdev = jnp.zeros((npower, 128), jnp.float32)
    for b in range(BINS):
        xdev = jnp.where(lane == b, deviations[b] / square, xdev)
    yfit = jnp.log(jnp.where(lane < BINS, table + 1.0 / genes_all, 1.0)) * LOG10E
    slope = jnp.sum(xdev * yfit, axis=1, keepdims=True)
    total = jnp.sum(jnp.where(lane == BINS, table, 0.0), axis=1, keepdims=True)
    mean_log = jnp.log(total) * LOG10E
    fit_ref[padded:padded + 1, :] = jnp.sum(jnp.where(lane == line, slope, 0.0), axis=0, keepdims=True)
    fit_ref[padded + 1:padded + 2, :] = jnp.sum(jnp.where(lane == line, mean_log, 0.0), axis=0, keepdims=True)


def unpack_kernel(npower, log_degree_in, fit_in, log_degree_ref, freq_ref, slope_ref, mean_log_ref):
    padded = fit_in.shape[0] - 8
    log_degree_ref[...] = log_degree_in[...]
    freq_ref[...] = fit_in[0:npower, :BINS]
    slope_ref[...] = fit_in[padded:padded + 1, :npower]
    mean_log_ref[...] = fit_in[padded + 1:padded + 2, :npower]


def solution(mesh):
    nr, nc = mesh.shape["row"], mesh.shape["col"]
    n1, n0 = split(nr // 2)
    nh, nl = split(nc)

    def on_device(expression, powers):
        genes, samples = expression.shape
        npower = powers.shape[0]
        nleft, npair = nh * n0, nl * n1
        height = -(-npower * nleft // 8) * 8
        vmem = pl.BlockSpec(memory_space=pltpu.VMEM)
        hbm = pl.BlockSpec(memory_space=pltpu.HBM)
        dma = pltpu.SemaphoreType.DMA
        f32 = jnp.float32
        padded = npower + 8 - npower % 8
        log_degree, packed = pl.pallas_call(
            functools.partial(kernel, n0, n1, nh, nl, npower),
            out_shape=(
                pltpu.VMEM((npower, genes), f32),
                pltpu.VMEM((padded + 8, 128), f32),
            ),
            in_specs=[hbm, hbm],
            out_specs=(vmem, vmem),
            scratch_shapes=[
                pltpu.SMEM((npower,), jnp.int32),
                pltpu.VMEM((nleft, genes, samples), jnp.bfloat16),
                pltpu.VMEM((npair, 2 * genes, samples), jnp.bfloat16),
                pltpu.VMEM((nleft + 2 * npair, 2, genes), f32),
                pltpu.VMEM((npair, 2 * genes, 128), f32),
                pltpu.VMEM((npair, 2 * genes, 128), f32),
                pltpu.VMEM((nleft, npair, 2 * genes, genes), f32),
                pltpu.VMEM((nleft, npower, 8, genes), f32),
                pltpu.VMEM((nleft * nleft, npower, genes), f32),
                pltpu.VMEM((2 * npair, height, genes), f32),
                dma((4,)),
                dma((3,)),
                dma((nh - 1, CHUNKS)),
                dma((nh, n0 - 1)),
                dma((nl - 1, CHUNKS)),
                dma((nl, n1 - 1, CHUNKS)),
                dma((nl, n1, 2)),
                dma((nleft + 2 * npair - 2,)),
                dma((3,)),
                dma((2,)),
            ],
            compiler_params=pltpu.CompilerParams(
                collective_id=0, has_side_effects=True, vmem_limit_bytes=67043328 - 128 * 1024
            ),
        )(powers, expression)
        log_degree, freq, slope, mean_log = pl.pallas_call(
            functools.partial(unpack_kernel, npower),
            out_shape=(
                jax.ShapeDtypeStruct((npower, genes), f32),
                jax.ShapeDtypeStruct((npower, BINS), f32),
                jax.ShapeDtypeStruct((1, npower), f32),
                jax.ShapeDtypeStruct((1, npower), f32),
            ),
            in_specs=[vmem, vmem],
            out_specs=(vmem,) * 4,
            compiler_params=pltpu.CompilerParams(vmem_limit_bytes=1 << 20),
        )(log_degree, packed)
        return log_degree, freq, slope.reshape(npower), mean_log.reshape(npower)

    return jax.shard_map(
        on_device,
        mesh=mesh,
        in_specs=(P(("row", "col"), None), P()),
        out_specs=(P(None, ("row", "col")), P(), P(), P()),
        check_vma=False,
    )
```

```python
import functools
import math

import jax
import jax.numpy as jnp
from jax import lax
from jax.experimental import pallas as pl
from jax.experimental.pallas import tpu as pltpu
from jax.sharding import PartitionSpec as P

BINS = 10
EDGES = (0, 2, 4, 6, 7, 8)
CHUNKS = len(EDGES) - 1
LATE = 2
STATS = CHUNKS
STRIP = 32
UNROLL = 2
LOG2E = math.log2(math.e)
LOG10E = math.log10(math.e)
MESH = pl.DeviceIdType.MESH


def split(size):
    low = max(f for f in range(1, math.isqrt(size) + 1) if size % f == 0)
    return size // low, low


def kernel(
    n0, n1, nh, nl, npower, powers_hbm, expr_hbm, log_degree_ref, fit_ref,
    powers_ref, left, right, stats, right_mean, right_inv, raw_ref, sums_ref, partial, degrees, degrees_sent,
    load_sem, send_sem,
    far_recv, side_recv, near_recv, up_recv, twin_recv, stat_recv, part_sem, deg_sem,
):
    r, c = lax.axis_index("row"), lax.axis_index("col")
    q, core = r // 2, r % 2
    q1, q0 = q // n0, q % n0
    ch, cl = c // nl, c % nl
    nleft, npair = nh * n0, nl * n1
    _, genes, samples = left.shape
    edges = [genes * e // EDGES[-1] for e in EDGES]
    late = 2 * edges[LATE]

    def device(d0=0, dh=0, d1=0, dl=0, other=False):
        row = (((q1 + d1) % n1) * n0 + (q0 + d0) % n0) * 2 + (1 - core if other else core)
        return row, ((ch + dh) % nh) * nl + (cl + dl) % nl

    def left_slot(dh, d0):
        return ((ch + nh - dh) % nh) * n0 + (q0 + n0 - d0) % n0

    def pair_slot(dl, d1):
        return ((cl + nl - dl) % nl) * n1 + (q1 + n1 - d1) % n1

    own_left, own_pair = left_slot(0, 0), pair_slot(0, 0)
    block = left.at[own_left]

    def left_piece(slot, k):
        if k == STATS:
            return stats.at[slot]
        return left.at[slot, pl.ds(edges[k], edges[k + 1] - edges[k])]

    def right_piece(slot, side, k):
        if k == STATS:
            return stats.at[nleft + slot * 2 + side]
        size = edges[k + 1] - edges[k]
        return right.at[slot, pl.ds(2 * edges[k] + side * size, size)]

    for k in range(CHUNKS):
        source = expr_hbm.at[pl.ds(edges[k], edges[k + 1] - edges[k])]
        pltpu.make_async_copy(source, right_piece(own_pair, core, k), load_sem.at[0 if k == 0 else 1]).start()
    loads = [
        pltpu.make_async_copy(expr_hbm, block, load_sem.at[2]),
        pltpu.make_async_copy(powers_hbm, powers_ref, load_sem.at[3]),
    ]
    for load in loads:
        load.start()

    barrier = pltpu.get_barrier_semaphore()
    greeted = [dict(other=True)]
    greeted += [dict(d0=d) for d in range(1, n0)]
    greeted += [dict(d1=d) for d in range(1, n1)]
    greeted += [dict(dh=d) for d in range(1, nh)]
    greeted += [dict(dl=d) for d in range(1, nl)]
    for where in greeted:
        pl.semaphore_signal(barrier, inc=1, device_id=device(**where), device_id_type=MESH)

    def load_wait(low, high, sem):
        window = pl.ds(edges[low], edges[high] - edges[low])
        pltpu.make_async_copy(expr_hbm.at[window], left.at[own_left, window], load_sem.at[sem]).wait()

    load_wait(0, 1, 0)
    pl.semaphore_wait(barrier, len(greeted))

    def remote(ref, send, recv, where, src=None):
        return pltpu.make_async_remote_copy(
            src_ref=ref if src is None else src, dst_ref=ref, send_sem=send, recv_sem=recv, device_id=device(**where), device_id_type=MESH
        )

    flows = [("far", dh, 0) for dh in range(1, nh)] + [("near", dl, 0) for dl in range(1, nl)]
    flows += [("side", dh, d0) for dh in range(nh) for d0 in range(1, n0)]
    flows += [("up", dl, d1) for dl in range(nl) for d1 in range(1, n1)]
    flows += [("twin", dl, d1) for dl in range(nl) for d1 in range(n1)]

    def sems(kind, a, b, k):
        if k == STATS:
            return send_sem.at[0], stat_recv.at[flows.index((kind, a, b))]
        if kind == "far":
            return send_sem.at[1], far_recv.at[a - 1, k]
        if kind == "near":
            return send_sem.at[1], near_recv.at[a - 1, k]
        if kind == "side":
            return send_sem.at[1], side_recv.at[a, b - 1]
        if kind == "up":
            return send_sem.at[2], up_recv.at[a, b - 1, k]
        return send_sem.at[2], twin_recv.at[a, b, int(k >= LATE)]

    def send(kind, a, b, k):
        if kind == "far":
            ref, where = left_piece(own_left, k), dict(dh=a)
        elif kind == "side":
            ref, where = left_piece(left_slot(a, 0), k), dict(d0=b)
        elif kind == "near":
            ref, where = right_piece(own_pair, core, k), dict(dl=a)
        elif kind == "up":
            ref, where = right_piece(pair_slot(a, 0), core, k), dict(d1=b)
        else:
            ref, where = right_piece(pair_slot(a, b), core, k), dict(other=True)
        own = right_piece(own_pair, core, k) if kind == "far" or (kind == "side" and a == 0) else None
        remote(ref, *sems(kind, a, b, k), where, own).start()

    def wait(kind, a, b, k, ref):
        remote(ref, *sems(kind, a, b, k), dict(other=True)).wait_recv()

    def wait_far(dh, k):
        wait("far", dh, 0, k, left_piece(left_slot(dh, 0), k))

    def wait_side(dh, d0, k):
        wait("side", dh, d0, k, left_piece(left_slot(dh, d0), k) if k == STATS else left.at[left_slot(dh, d0)])

    def wait_near(dl, k):
        wait("near", dl, 0, k, right_piece(pair_slot(dl, 0), core, k))

    def wait_up(dl, d1, k):
        wait("up", dl, d1, k, right_piece(pair_slot(dl, d1), core, k))

    def wait_twin(dl, d1, k):
        slot = pair_slot(dl, d1)
        if k == STATS:
            ref = right_piece(slot, 1 - core, k)
        else:
            ref = right.at[slot, pl.ds(0, edges[LATE]) if k < LATE else pl.ds(late, genes - edges[LATE])]
        wait("twin", dl, d1, k, ref)

    def send_own(k):
        for first in (0, 1):
            @pl.when(core == first)
            def _():
                for kind in ("far", "near") if first == 0 else ("near", "far"):
                    for a in range(1, nh if kind == "far" else nl):
                        send(kind, a, 0, k)

        for d0 in range(1, n0):
            send("side", 0, d0, k)
        for d1 in range(1, n1):
            send("up", 0, d1, k)
        send("twin", 0, 0, k)

    send_own(0)
    load_wait(1, CHUNKS, 1)
    for load in loads:
        load.wait()
    values = left[own_left].astype(jnp.float32)
    mean = jnp.mean(values, axis=1, keepdims=True)
    centred = values - mean
    inv = lax.rsqrt(jnp.mean(centred * centred, axis=1, keepdims=True) + 1e-06)
    own_stats = jnp.concatenate(
        [jnp.broadcast_to(mean, (genes, 128)).T[0:1, :], jnp.broadcast_to(inv, (genes, 128)).T[0:1, :]], axis=0
    )
    stats[own_left] = own_stats
    stats[nleft + own_pair * 2 + core] = own_stats
    for k in (STATS, *range(1, CHUNKS)):
        send_own(k)
    for slot in range(nleft):
        for p in range(npower):
            sums_ref[slot, p] = jnp.zeros((8, genes), jnp.float32)
    exponents = [powers_ref[p].astype(jnp.float32) * LOG2E for p in range(npower)]

    def multiply(ls, blocks, ps, pairs, lo=0, hi=2 * genes):
        size = hi - lo
        lhs = right[pl.ds(ps, pairs), lo:hi].reshape(pairs * size, samples)
        rhs = left[pl.ds(ls, blocks)].reshape(blocks * genes, samples)
        raw = lax.dot_general(lhs, rhs, (((1,), (1,)), ((), ())), preferred_element_type=jnp.float32)
        for a in range(blocks):
            for b in range(pairs):
                raw_ref[ls + a, ps + b, lo:hi] = raw[b * size:(b + 1) * size, a * genes:(a + 1) * genes]

    def accumulate(ls, ps, lo=0, hi=2 * genes):
        mean_row, inv_row = stats[ls, 0:1, :], stats[ls, 1:2, :]
        totals = [None] * npower
        for s in range(lo, hi, STRIP):
            raw = raw_ref[ls, ps, s:s + STRIP, :]
            mean_col, inv_col = right_mean[ps, s:s + STRIP, :], right_inv[ps, s:s + STRIP, :]
            pearson = (raw * (1.0 / samples) - mean_col * mean_row) * inv_col * inv_row
            log_abs = jnp.log(jnp.abs(pearson))
            for p in range(npower):
                part = jnp.sum(jnp.exp2(exponents[p] * log_abs).reshape(STRIP // 8, 8, genes), axis=0)
                totals[p] = part if totals[p] is None else totals[p] + part
        for p in range(npower):
            sums_ref[ls, p] = sums_ref[ls, p] + totals[p]

    def part(ls, blocks, ps, pairs, lo=0, hi=2 * genes):
        return ls, blocks, ps, pairs, lo, hi

    def run(*parts):
        multiply(*parts[0])
        for each, later in zip(parts, parts[1:] + (None,)):
            if later is not None:
                multiply(*later)
            add(*each)

    def add(ls, blocks, ps, pairs, lo=0, hi=2 * genes):
        def body(u, _):
            accumulate(ls + lax.rem(u, blocks), ps + lax.div(u, blocks), lo, hi)
            return 0

        if blocks * pairs <= 4:
            for u in range(blocks * pairs):
                accumulate(ls + u % blocks, ps + u // blocks, lo, hi)
        else:
            lax.fori_loop(0, blocks * pairs, body, 0, unroll=UNROLL)

    def columns(dl, d1):
        slot = pair_slot(dl, d1)
        for side in (0, 1):
            row = stats[nleft + slot * 2 + side]
            mean_col = jnp.broadcast_to(row[0:1], (128, genes)).T
            inv_col = jnp.broadcast_to(row[1:2], (128, genes)).T
            for k in range(CHUNKS):
                low, high = edges[k], edges[k + 1]
                window = pl.ds(2 * low + side * (high - low), high - low)
                right_mean[slot, window] = mean_col[low:high]
                right_inv[slot, window] = inv_col[low:high]

    own_row, own_line = ch * n0, cl * n1
    far_pairs = [(dl, 0) for dl in range(1, nl)]
    rest_pairs = [(dl, d1) for dl in range(1, nl) for d1 in range(1, n1)]
    far_rows = [(ch + nh - dh) % nh * n0 for dh in range(1, nh)]
    far_blocks = [left_slot(dh, 0) for dh in range(1, nh)]
    rest_blocks = [(dh, d0) for dh in range(1, nh) for d0 in range(1, n0)]

    early_blocks = [(0, d0) for d0 in range(n0)]
    late_blocks = [(dh, d0) for dh in range(1, nh) for d0 in range(n0)]
    far_lines = [(cl + nl - dl) % nl * n1 for dl in range(1, nl)]

    def index_of(a, b, side, dh, d0):
        return ((a * n0 + b) * 2 + side) * nleft + dh * n0 + d0

    def send_partials(group):
        count = len(group)
        blocks = [
            jnp.concatenate([jnp.sum(sums_ref[left_slot(*m), p], axis=0, keepdims=True) for p in range(npower)], axis=0)
            for m in group
        ]
        for side in (0, 1):
            first = index_of(0, 0, side, *group[0])

            @pl.when(core == side)
            def _():
                for i in range(count):
                    partial[first + i] = blocks[i]
                for a in reversed(range(nh)):
                    for b in reversed(range(n0)):
                        if a or b or side == 0:
                            pltpu.make_async_remote_copy(
                                src_ref=partial.at[pl.ds(first, count)],
                                dst_ref=partial.at[pl.ds(index_of(a, b, side, *group[0]), count)],
                                send_sem=part_sem.at[0], recv_sem=part_sem.at[1 if group is early_blocks else 2],
                                device_id=device(dh=a, d0=b, other=side == 0), device_id_type=MESH,
                            ).start()

    def pass_up(k):
        for d1 in range(1, n1):
            wait_up(0, d1, k)
            send("twin", 0, d1, k)

    def pass_far(k):
        for dl in range(1, nl):
            wait_near(dl, k)
            for d1 in range(1, n1):
                send("up", dl, d1, k)
            send("twin", dl, 0, k)
        for dh in range(1, nh):
            wait_far(dh, k)
            for d0 in range(1, n0):
                send("side", dh, d0, k)

    def pass_rest(k):
        for dl, d1 in rest_pairs:
            wait_up(dl, d1, k)
            send("twin", dl, d1, k)

    wait_twin(0, 0, STATS)
    wait_twin(0, 0, 0)
    wait_twin(0, 0, LATE)
    columns(0, 0)
    pass_up(0)
    pass_up(STATS)
    pass_up(1)
    pass_far(0)
    pass_far(STATS)
    for k in range(2, CHUNKS):
        pass_up(k)
    for d1 in range(1, n1):
        wait_twin(0, d1, STATS)
        columns(0, d1)
    for d0 in range(1, n0):
        wait_side(0, d0, STATS)
        wait_side(0, d0, 0)
    pass_far(1)
    run(part(own_row, n0, own_pair, 1))
    for d1 in range(1, n1):
        wait_twin(0, d1, 0)
        wait_twin(0, d1, LATE)
        run(part(own_row, n0, pair_slot(0, d1), 1))
    pass_rest(STATS)
    pass_rest(0)
    pass_far(2)
    for m in far_pairs:
        wait_twin(*m, STATS)
        columns(*m)
        wait_twin(*m, 0)
    run(*[part(own_row, n0, pair_slot(*m), 1, 0, late) for m in far_pairs])
    for m in rest_pairs:
        wait_twin(*m, STATS)
        columns(*m)
    for dh in range(1, nh):
        for d0 in range(1, n0):
            wait_side(dh, d0, STATS)
    pass_rest(1)
    pass_far(3)
    for k in range(4, CHUNKS):
        pass_far(k)
    run(*[part(b, 1, own_line, n1) for b in far_blocks])
    for m in far_pairs:
        wait_twin(*m, LATE)
    for m in rest_pairs:
        wait_twin(*m, 0)
    run(
        *[part(b, 1, pair_slot(*m), 1) for b in far_blocks for m in far_pairs],
        *[part(own_row, n0, pair_slot(*m), 1, late) for m in far_pairs],
        *[part(own_row, n0, pair_slot(*m), 1, 0, late) for m in rest_pairs],
        *[part(b, 1, pair_slot(*m), 1, 0, late) for b in far_blocks for m in rest_pairs],
    )
    for k in range(2, CHUNKS):
        pass_rest(k)
    for m in rest_blocks:
        wait_side(*m, 0)
    run(
        *[part(left_slot(*b), 1, own_line, n1) for b in rest_blocks],
        *[part(left_slot(*b), 1, pair_slot(*m), 1) for b in rest_blocks for m in far_pairs],
        *[part(left_slot(*b), 1, pair_slot(*m), 1, 0, late) for b in rest_blocks for m in rest_pairs],
    )
    for m in rest_pairs:
        wait_twin(*m, LATE)
    for m in rest_pairs:
        multiply(0, nleft, pair_slot(*m), 1, late)
    for m in rest_pairs:
        add(own_row, n0, pair_slot(*m), 1, late)
    send_partials(early_blocks)
    for m in rest_pairs:
        for b in far_rows:
            add(b, n0, pair_slot(*m), 1, late)

    send_partials(late_blocks)

    @pl.when(core == 1)
    def _():
        for group, sem in ((early_blocks, 1), (late_blocks, 2)):
            if group:
                arrived = partial.at[pl.ds(0, (2 * nleft - 1) * len(group))]
                remote(arrived, part_sem.at[0], part_sem.at[sem], dict(other=True)).wait_recv()
        lines = []
        for side in (0, 1):
            for dh in range(nh):
                for d0 in range(n0):
                    total = None
                    for a in range(nh):
                        for b in range(n0):
                            term = partial[index_of(a, b, side, (dh - a) % nh, (d0 - b) % n0)]
                            total = term if total is None else total + term
                    lines.append(total)
        height = degrees.shape[1]
        if height > 2 * nleft * npower:
            lines.append(jnp.zeros((height - 2 * nleft * npower, genes), jnp.float32))
        degrees[own_pair] = jnp.concatenate(lines, axis=0)
        for dl in reversed(range(nl)):
            for d1 in reversed(range(n1)):
                for o in (True, False):
                    if dl or d1 or o:
                        where = dict(dl=dl, d1=d1, other=o)
                        remote(degrees.at[own_pair], deg_sem.at[0], deg_sem.at[1], where).start()

    pair_flows = [flow for flow in flows if flow[0] in ("up", "twin")]
    pairs_ref = right.reshape(2 * npair, genes, samples)
    for group in ([flow for flow in flows if flow not in pair_flows], pair_flows):
        remote(pairs_ref.at[pl.ds(0, len(group))], *sems(*group[0], 0), dict(other=True)).wait_send()
    remote(stats.at[pl.ds(0, len(flows))], *sems(*flows[0], STATS), dict(other=True)).wait_send()
    for side in (0, 1):
        @pl.when(core == side)
        def _():
            sent = partial.at[pl.ds(0, (nleft - side) * nleft)]
            remote(sent, part_sem.at[0], part_sem.at[1], dict(other=True)).wait_send()
            if npair > side:
                arrived = degrees.at[pl.ds(0, npair - side)]
                remote(arrived, deg_sem.at[0], deg_sem.at[1], dict(other=True)).wait_recv()

    fit(genes * nleft * npair * 2, 2 * nleft, npower, degrees, fit_ref)
    mine = degrees[own_pair, 0:npower]
    mine = jnp.where(core == 1, degrees[own_pair, nleft * npower:(nleft + 1) * npower], mine)
    log_degree_ref[...] = jnp.log(mine) * LOG10E

    @pl.when(core == 1)
    def _():
        remote(degrees_sent.at[pl.ds(0, 2 * npair - 1)], deg_sem.at[0], deg_sem.at[1], dict(other=True)).wait_send()


def fit(genes_all, nleft, npower, degrees, fit_ref):
    blocks, height, genes = degrees.shape
    padded = fit_ref.shape[0] - 8

    def fold(values, combine):
        total = values[:npower]
        for block in range(1, nleft):
            total = combine(total, values[block * npower:(block + 1) * npower])
        return total

    best = degrees[0]
    for index in range(1, blocks):
        best = jnp.maximum(best, degrees[index])
    best = jnp.broadcast_to(jnp.max(best, axis=1, keepdims=True), (height, genes))
    scales = [BINS / fold(best, jnp.maximum)] * nleft
    if height > nleft * npower:
        scales.append(jnp.ones((height - nleft * npower, genes), jnp.float32))
    scale = jnp.concatenate(scales, axis=0)
    positions = [jnp.clip(degrees[index] * scale - 0.5, 0.0, BINS - 1.0) for index in range(blocks)]
    lane = lax.broadcasted_iota(jnp.int32, (height, 128), 1)
    table = jnp.zeros((height, 128), jnp.float32)
    for b in range(BINS + 1):
        total = None
        for index in range(blocks):
            term = degrees[index] if b == BINS else jnp.maximum(0.0, 1.0 - jnp.abs(positions[index] - b))
            total = term if total is None else total + term
        table = jnp.where(lane == b, jnp.sum(total, axis=1, keepdims=True), table)
    table = fold(table, jnp.add) / genes_all
    fit_ref[0:npower, :] = table
    lane = lax.broadcasted_iota(jnp.int32, (npower, 128), 1)
    line = lax.broadcasted_iota(jnp.int32, (npower, 128), 0)
    logs = [math.log10(b + 0.5) for b in range(BINS)]
    deviations = [value - sum(logs) / BINS for value in logs]
    square = sum(value * value for value in deviations)
    xdev = jnp.zeros((npower, 128), jnp.float32)
    for b in range(BINS):
        xdev = jnp.where(lane == b, deviations[b] / square, xdev)
    yfit = jnp.log(jnp.where(lane < BINS, table + 1.0 / genes_all, 1.0)) * LOG10E
    slope = jnp.sum(xdev * yfit, axis=1, keepdims=True)
    total = jnp.sum(jnp.where(lane == BINS, table, 0.0), axis=1, keepdims=True)
    mean_log = jnp.log(total) * LOG10E
    fit_ref[padded:padded + 1, :] = jnp.sum(jnp.where(lane == line, slope, 0.0), axis=0, keepdims=True)
    fit_ref[padded + 1:padded + 2, :] = jnp.sum(jnp.where(lane == line, mean_log, 0.0), axis=0, keepdims=True)


def unpack_kernel(npower, log_degree_in, fit_in, log_degree_ref, freq_ref, slope_ref, mean_log_ref):
    padded = fit_in.shape[0] - 8
    log_degree_ref[...] = log_degree_in[...]
    freq_ref[...] = fit_in[0:npower, :BINS]
    slope_ref[...] = fit_in[padded:padded + 1, :npower]
    mean_log_ref[...] = fit_in[padded + 1:padded + 2, :npower]


def solution(mesh):
    nr, nc = mesh.shape["row"], mesh.shape["col"]
    n1, n0 = split(nr // 2)
    nh, nl = split(nc)

    def on_device(expression, powers):
        genes, samples = expression.shape
        npower = powers.shape[0]
        nleft, npair = nh * n0, nl * n1
        height = -(-2 * npower * nleft // 8) * 8
        vmem = pl.BlockSpec(memory_space=pltpu.VMEM)
        hbm = pl.BlockSpec(memory_space=pltpu.HBM)
        dma = pltpu.SemaphoreType.DMA
        f32 = jnp.float32
        padded = npower + 8 - npower % 8
        log_degree, packed = pl.pallas_call(
            functools.partial(kernel, n0, n1, nh, nl, npower),
            out_shape=(
                pltpu.VMEM((npower, genes), f32),
                pltpu.VMEM((padded + 8, 128), f32),
            ),
            in_specs=[hbm, hbm],
            out_specs=(vmem, vmem),
            scratch_shapes=[
                pltpu.SMEM((npower,), jnp.int32),
                pltpu.VMEM((nleft, genes, samples), jnp.bfloat16),
                pltpu.VMEM((npair, 2 * genes, samples), jnp.bfloat16),
                pltpu.VMEM((nleft + 2 * npair, 2, genes), f32),
                pltpu.VMEM((npair, 2 * genes, 128), f32),
                pltpu.VMEM((npair, 2 * genes, 128), f32),
                pltpu.VMEM((nleft, npair, 2 * genes, genes), f32),
                pltpu.VMEM((nleft, npower, 8, genes), f32),
                pltpu.VMEM((2 * nleft * nleft, npower, genes), f32),
                pltpu.VMEM((npair, height, genes), f32),
                pltpu.VMEM((2 * npair - 1, height, genes), f32),
                dma((4,)),
                dma((3,)),
                dma((nh - 1, CHUNKS)),
                dma((nh, n0 - 1)),
                dma((nl - 1, CHUNKS)),
                dma((nl, n1 - 1, CHUNKS)),
                dma((nl, n1, 2)),
                dma((nleft + 2 * npair - 2,)),
                dma((3,)),
                dma((2,)),
            ],
            compiler_params=pltpu.CompilerParams(
                collective_id=0, has_side_effects=True, vmem_limit_bytes=67043328 - 128 * 1024
            ),
        )(powers, expression)
        log_degree, freq, slope, mean_log = pl.pallas_call(
            functools.partial(unpack_kernel, npower),
            out_shape=(
                jax.ShapeDtypeStruct((npower, genes), f32),
                jax.ShapeDtypeStruct((npower, BINS), f32),
                jax.ShapeDtypeStruct((1, npower), f32),
                jax.ShapeDtypeStruct((1, npower), f32),
            ),
            in_specs=[vmem, vmem],
            out_specs=(vmem,) * 4,
            compiler_params=pltpu.CompilerParams(vmem_limit_bytes=1 << 20),
        )(log_degree, packed)
        return log_degree, freq, slope.reshape(npower), mean_log.reshape(npower)

    return jax.shard_map(
        on_device,
        mesh=mesh,
        in_specs=(P(("row", "col"), None), P()),
        out_specs=(P(None, ("row", "col")), P(), P(), P()),
        check_vma=False,
    )
```

```python
import functools
import math

import jax
import jax.numpy as jnp
from jax import lax
from jax.experimental import pallas as pl
from jax.experimental.pallas import tpu as pltpu
from jax.sharding import PartitionSpec as P

BINS = 10
EDGES = (0, 2, 4, 6, 7, 8)
CHUNKS = len(EDGES) - 1
LATE = 2
STATS = CHUNKS
STRIP = 32
UNROLL = 2
LOG2E = math.log2(math.e)
LOG10E = math.log10(math.e)
MESH = pl.DeviceIdType.MESH


def split(size):
    low = max(f for f in range(1, math.isqrt(size) + 1) if size % f == 0)
    return size // low, low


def kernel(
    n0, n1, nh, nl, npower, powers_hbm, expr_hbm, log_degree_ref, fit_ref,
    powers_ref, left, right, stats, right_mean, right_inv, raw_ref, sums_ref, partial, degrees, degrees_sent,
    load_sem, send_sem,
    far_recv, side_recv, near_recv, up_recv, twin_recv, stat_recv, part_sem, deg_sem,
):
    r, c = lax.axis_index("row"), lax.axis_index("col")
    q, core = r // 2, r % 2
    q1, q0 = q // n0, q % n0
    ch, cl = c // nl, c % nl
    nleft, npair = nh * n0, nl * n1
    _, genes, samples = left.shape
    edges = [genes * e // EDGES[-1] for e in EDGES]
    late = 2 * edges[LATE]

    def device(d0=0, dh=0, d1=0, dl=0, other=False):
        row = (((q1 + d1) % n1) * n0 + (q0 + d0) % n0) * 2 + (1 - core if other else core)
        return row, ((ch + dh) % nh) * nl + (cl + dl) % nl

    def left_slot(dh, d0):
        return ((ch + nh - dh) % nh) * n0 + (q0 + n0 - d0) % n0

    def pair_slot(dl, d1):
        return ((cl + nl - dl) % nl) * n1 + (q1 + n1 - d1) % n1

    own_left, own_pair = left_slot(0, 0), pair_slot(0, 0)
    block = left.at[own_left]

    def left_piece(slot, k):
        if k == STATS:
            return stats.at[slot]
        return left.at[slot, pl.ds(edges[k], edges[k + 1] - edges[k])]

    def right_piece(slot, side, k):
        if k == STATS:
            return stats.at[nleft + slot * 2 + side]
        size = edges[k + 1] - edges[k]
        return right.at[slot, pl.ds(2 * edges[k] + side * size, size)]

    for k in range(CHUNKS):
        source = expr_hbm.at[pl.ds(edges[k], edges[k + 1] - edges[k])]
        pltpu.make_async_copy(source, right_piece(own_pair, core, k), load_sem.at[0 if k == 0 else 1]).start()
    loads = [
        pltpu.make_async_copy(expr_hbm, block, load_sem.at[2]),
        pltpu.make_async_copy(powers_hbm, powers_ref, load_sem.at[3]),
    ]
    for load in loads:
        load.start()

    barrier = pltpu.get_barrier_semaphore()
    greeted = [dict(other=True)]
    greeted += [dict(d0=d) for d in range(1, n0)]
    greeted += [dict(d1=d) for d in range(1, n1)]
    greeted += [dict(dh=d) for d in range(1, nh)]
    greeted += [dict(dl=d) for d in range(1, nl)]
    for where in greeted:
        pl.semaphore_signal(barrier, inc=1, device_id=device(**where), device_id_type=MESH)

    def load_wait(low, high, sem):
        window = pl.ds(edges[low], edges[high] - edges[low])
        pltpu.make_async_copy(expr_hbm.at[window], left.at[own_left, window], load_sem.at[sem]).wait()

    load_wait(0, 1, 0)
    pl.semaphore_wait(barrier, len(greeted))

    def remote(ref, send, recv, where, src=None):
        return pltpu.make_async_remote_copy(
            src_ref=ref if src is None else src, dst_ref=ref, send_sem=send, recv_sem=recv, device_id=device(**where), device_id_type=MESH
        )

    flows = [("far", dh, 0) for dh in range(1, nh)] + [("near", dl, 0) for dl in range(1, nl)]
    flows += [("side", dh, d0) for dh in range(nh) for d0 in range(1, n0)]
    flows += [("up", dl, d1) for dl in range(nl) for d1 in range(1, n1)]
    flows += [("twin", dl, d1) for dl in range(nl) for d1 in range(n1)]

    def sems(kind, a, b, k):
        if k == STATS:
            return send_sem.at[0], stat_recv.at[flows.index((kind, a, b))]
        if kind == "far":
            return send_sem.at[1], far_recv.at[a - 1, k]
        if kind == "near":
            return send_sem.at[1], near_recv.at[a - 1, k]
        if kind == "side":
            return send_sem.at[1], side_recv.at[a, b - 1]
        if kind == "up":
            return send_sem.at[2], up_recv.at[a, b - 1, k]
        return send_sem.at[2], twin_recv.at[a, b, int(k >= LATE)]

    def send(kind, a, b, k):
        if kind == "far":
            ref, where = left_piece(own_left, k), dict(dh=a)
        elif kind == "side":
            ref, where = left_piece(left_slot(a, 0), k), dict(d0=b)
        elif kind == "near":
            ref, where = right_piece(own_pair, core, k), dict(dl=a)
        elif kind == "up":
            ref, where = right_piece(pair_slot(a, 0), core, k), dict(d1=b)
        else:
            ref, where = right_piece(pair_slot(a, b), core, k), dict(other=True)
        own = right_piece(own_pair, core, k) if kind == "far" or (kind == "side" and a == 0) else None
        remote(ref, *sems(kind, a, b, k), where, own).start()

    def wait(kind, a, b, k, ref):
        remote(ref, *sems(kind, a, b, k), dict(other=True)).wait_recv()

    def wait_far(dh, k):
        wait("far", dh, 0, k, left_piece(left_slot(dh, 0), k))

    def wait_side(dh, d0, k):
        wait("side", dh, d0, k, left_piece(left_slot(dh, d0), k) if k == STATS else left.at[left_slot(dh, d0)])

    def wait_near(dl, k):
        wait("near", dl, 0, k, right_piece(pair_slot(dl, 0), core, k))

    def wait_up(dl, d1, k):
        wait("up", dl, d1, k, right_piece(pair_slot(dl, d1), core, k))

    def wait_twin(dl, d1, k):
        slot = pair_slot(dl, d1)
        if k == STATS:
            ref = right_piece(slot, 1 - core, k)
        else:
            ref = right.at[slot, pl.ds(0, edges[LATE]) if k < LATE else pl.ds(late, genes - edges[LATE])]
        wait("twin", dl, d1, k, ref)

    def send_own(k):
        for first in (0, 1):
            @pl.when(core == first)
            def _():
                for kind in ("far", "near") if first == 0 else ("near", "far"):
                    for a in range(1, nh if kind == "far" else nl):
                        send(kind, a, 0, k)

        for d0 in range(1, n0):
            send("side", 0, d0, k)
        for d1 in range(1, n1):
            send("up", 0, d1, k)
        send("twin", 0, 0, k)

    send_own(0)
    load_wait(1, CHUNKS, 1)
    for load in loads:
        load.wait()
    values = left[own_left].astype(jnp.float32)
    mean = jnp.mean(values, axis=1, keepdims=True)
    centred = values - mean
    inv = lax.rsqrt(jnp.mean(centred * centred, axis=1, keepdims=True) + 1e-06)
    own_stats = jnp.concatenate(
        [jnp.broadcast_to(mean, (genes, 128)).T[0:1, :], jnp.broadcast_to(inv, (genes, 128)).T[0:1, :]], axis=0
    )
    stats[own_left] = own_stats
    stats[nleft + own_pair * 2 + core] = own_stats
    for k in (STATS, *range(1, CHUNKS)):
        send_own(k)
    for slot in range(nleft):
        for p in range(npower):
            sums_ref[slot, p] = jnp.zeros((8, genes), jnp.float32)
    exponents = [powers_ref[p].astype(jnp.float32) * LOG2E for p in range(npower)]

    def multiply(ls, blocks, ps, pairs, lo=0, hi=2 * genes):
        size = hi - lo
        lhs = right[pl.ds(ps, pairs), lo:hi].reshape(pairs * size, samples)
        rhs = left[pl.ds(ls, blocks)].reshape(blocks * genes, samples)
        raw = lax.dot_general(lhs, rhs, (((1,), (1,)), ((), ())), preferred_element_type=jnp.float32)
        for a in range(blocks):
            for b in range(pairs):
                raw_ref[ls + a, ps + b, lo:hi] = raw[b * size:(b + 1) * size, a * genes:(a + 1) * genes]

    def accumulate(ls, ps, lo=0, hi=2 * genes):
        mean_row, inv_row = stats[ls, 0:1, :], stats[ls, 1:2, :]
        totals = [None] * npower
        for s in range(lo, hi, STRIP):
            raw = raw_ref[ls, ps, s:s + STRIP, :]
            mean_col, inv_col = right_mean[ps, s:s + STRIP, :], right_inv[ps, s:s + STRIP, :]
            pearson = (raw * (1.0 / samples) - mean_col * mean_row) * inv_col * inv_row
            log_abs = jnp.log(jnp.abs(pearson))
            for p in range(npower):
                part = jnp.sum(jnp.exp2(exponents[p] * log_abs).reshape(STRIP // 8, 8, genes), axis=0)
                totals[p] = part if totals[p] is None else totals[p] + part
        for p in range(npower):
            sums_ref[ls, p] = sums_ref[ls, p] + totals[p]

    def part(ls, blocks, ps, pairs, lo=0, hi=2 * genes):
        return ls, blocks, ps, pairs, lo, hi

    def run(*parts):
        multiply(*parts[0])
        for each, later in zip(parts, parts[1:] + (None,)):
            if later is not None:
                multiply(*later)
            add(*each)

    def add(ls, blocks, ps, pairs, lo=0, hi=2 * genes):
        def body(u, _):
            accumulate(ls + lax.rem(u, blocks), ps + lax.div(u, blocks), lo, hi)
            return 0

        if blocks * pairs <= 4:
            for u in range(blocks * pairs):
                accumulate(ls + u % blocks, ps + u // blocks, lo, hi)
        else:
            lax.fori_loop(0, blocks * pairs, body, 0, unroll=UNROLL)

    def columns(dl, d1):
        slot = pair_slot(dl, d1)
        for side in (0, 1):
            row = stats[nleft + slot * 2 + side]
            mean_col = jnp.broadcast_to(row[0:1], (128, genes)).T
            inv_col = jnp.broadcast_to(row[1:2], (128, genes)).T
            for k in range(CHUNKS):
                low, high = edges[k], edges[k + 1]
                window = pl.ds(2 * low + side * (high - low), high - low)
                right_mean[slot, window] = mean_col[low:high]
                right_inv[slot, window] = inv_col[low:high]

    own_row, own_line = ch * n0, cl * n1
    far_pairs = [(dl, 0) for dl in range(1, nl)]
    rest_pairs = [(dl, d1) for dl in range(1, nl) for d1 in range(1, n1)]
    far_rows = [(ch + nh - dh) % nh * n0 for dh in range(1, nh)]
    far_blocks = [left_slot(dh, 0) for dh in range(1, nh)]
    rest_blocks = [(dh, d0) for dh in range(1, nh) for d0 in range(1, n0)]

    early_blocks = [(0, d0) for d0 in range(n0)]
    late_blocks = [(dh, d0) for dh in range(1, nh) for d0 in range(n0)]
    far_lines = [(cl + nl - dl) % nl * n1 for dl in range(1, nl)]

    def index_of(a, b, side, dh, d0):
        return ((a * n0 + b) * 2 + side) * nleft + dh * n0 + d0

    def send_partials(group):
        count = len(group)
        blocks = [
            jnp.concatenate([jnp.sum(sums_ref[left_slot(*m), p], axis=0, keepdims=True) for p in range(npower)], axis=0)
            for m in group
        ]
        for side in (0, 1):
            first = index_of(0, 0, side, *group[0])

            @pl.when(core == side)
            def _():
                for i in range(count):
                    partial[first + i] = blocks[i]
                for a in reversed(range(nh)):
                    for b in reversed(range(n0)):
                        if a or b or side == 0:
                            pltpu.make_async_remote_copy(
                                src_ref=partial.at[pl.ds(first, count)],
                                dst_ref=partial.at[pl.ds(index_of(a, b, side, *group[0]), count)],
                                send_sem=part_sem.at[0], recv_sem=part_sem.at[1 if group is early_blocks else 2],
                                device_id=device(dh=a, d0=b, other=side == 0), device_id_type=MESH,
                            ).start()

    def pass_up(k):
        for d1 in range(1, n1):
            wait_up(0, d1, k)
            send("twin", 0, d1, k)

    def pass_far(k):
        for dl in range(1, nl):
            wait_near(dl, k)
            for d1 in range(1, n1):
                send("up", dl, d1, k)
            send("twin", dl, 0, k)
        for dh in range(1, nh):
            wait_far(dh, k)
            for d0 in range(1, n0):
                send("side", dh, d0, k)

    def pass_rest(k):
        for dl, d1 in rest_pairs:
            wait_up(dl, d1, k)
            send("twin", dl, d1, k)

    wait_twin(0, 0, STATS)
    wait_twin(0, 0, 0)
    wait_twin(0, 0, LATE)
    columns(0, 0)
    pass_up(0)
    pass_up(STATS)
    pass_up(1)
    pass_far(0)
    pass_far(STATS)
    for k in range(2, CHUNKS):
        pass_up(k)
    for d1 in range(1, n1):
        wait_twin(0, d1, STATS)
        columns(0, d1)
    for d0 in range(1, n0):
        wait_side(0, d0, STATS)
        wait_side(0, d0, 0)
    pass_far(1)
    run(part(own_row, n0, own_pair, 1))
    for d1 in range(1, n1):
        wait_twin(0, d1, 0)
        wait_twin(0, d1, LATE)
        run(part(own_row, n0, pair_slot(0, d1), 1))
    pass_rest(STATS)
    pass_rest(0)
    pass_far(2)
    for m in far_pairs:
        wait_twin(*m, STATS)
        columns(*m)
        wait_twin(*m, 0)
    run(*[part(own_row, n0, pair_slot(*m), 1, 0, late) for m in far_pairs])
    for m in rest_pairs:
        wait_twin(*m, STATS)
        columns(*m)
    for dh in range(1, nh):
        for d0 in range(1, n0):
            wait_side(dh, d0, STATS)
    pass_rest(1)
    pass_far(3)
    for k in range(4, CHUNKS):
        pass_far(k)
    run(*[part(b, 1, own_line, n1) for b in far_blocks])
    for m in far_pairs:
        wait_twin(*m, LATE)
    for m in rest_pairs:
        wait_twin(*m, 0)
    run(
        *[part(b, 1, pair_slot(*m), 1) for b in far_blocks for m in far_pairs],
        *[part(own_row, n0, pair_slot(*m), 1, late) for m in far_pairs],
        *[part(own_row, n0, pair_slot(*m), 1, 0, late) for m in rest_pairs],
        *[part(b, 1, pair_slot(*m), 1, 0, late) for b in far_blocks for m in rest_pairs],
    )
    for k in range(2, CHUNKS):
        pass_rest(k)
    for m in rest_blocks:
        wait_side(*m, 0)
    run(
        *[part(left_slot(*b), 1, own_line, n1) for b in rest_blocks],
        *[part(left_slot(*b), 1, pair_slot(*m), 1) for b in rest_blocks for m in far_pairs],
        *[part(left_slot(*b), 1, pair_slot(*m), 1, 0, late) for b in rest_blocks for m in rest_pairs],
    )
    for m in rest_pairs:
        wait_twin(*m, LATE)
    for m in rest_pairs:
        multiply(0, nleft, pair_slot(*m), 1, late)
    for m in rest_pairs:
        add(own_row, n0, pair_slot(*m), 1, late)
    send_partials(early_blocks)
    for m in rest_pairs:
        for b in far_rows:
            add(b, n0, pair_slot(*m), 1, late)

    send_partials(late_blocks)

    @pl.when(core == 1)
    def _():
        for group, sem in ((early_blocks, 1), (late_blocks, 2)):
            if group:
                arrived = partial.at[pl.ds(0, (2 * nleft - 1) * len(group))]
                remote(arrived, part_sem.at[0], part_sem.at[sem], dict(other=True)).wait_recv()
        lines = []
        for side in (0, 1):
            for dh in range(nh):
                for d0 in range(n0):
                    total = None
                    for a in range(nh):
                        for b in range(n0):
                            term = partial[index_of(a, b, side, (dh - a) % nh, (d0 - b) % n0)]
                            total = term if total is None else total + term
                    lines.append(total)
        height = degrees.shape[1]
        if height > 2 * nleft * npower:
            lines.append(jnp.zeros((height - 2 * nleft * npower, genes), jnp.float32))
        degrees[own_pair] = jnp.concatenate(lines, axis=0)
        for o in (True, False):
            for dl in reversed(range(nl)):
                for d1 in reversed(range(n1)):
                    if dl or d1 or o:
                        where = dict(dl=dl, d1=d1, other=o)
                        remote(degrees.at[own_pair], deg_sem.at[0], deg_sem.at[1], where).start()

    pair_flows = [flow for flow in flows if flow[0] in ("up", "twin")]
    pairs_ref = right.reshape(2 * npair, genes, samples)
    for group in ([flow for flow in flows if flow not in pair_flows], pair_flows):
        remote(pairs_ref.at[pl.ds(0, len(group))], *sems(*group[0], 0), dict(other=True)).wait_send()
    remote(stats.at[pl.ds(0, len(flows))], *sems(*flows[0], STATS), dict(other=True)).wait_send()
    for side in (0, 1):
        @pl.when(core == side)
        def _():
            sent = partial.at[pl.ds(0, (nleft - side) * nleft)]
            remote(sent, part_sem.at[0], part_sem.at[1], dict(other=True)).wait_send()
            if npair > side:
                arrived = degrees.at[pl.ds(0, npair - side)]
                remote(arrived, deg_sem.at[0], deg_sem.at[1], dict(other=True)).wait_recv()

    fit(genes * nleft * npair * 2, 2 * nleft, npower, degrees, fit_ref)
    mine = degrees[own_pair, 0:npower]
    mine = jnp.where(core == 1, degrees[own_pair, nleft * npower:(nleft + 1) * npower], mine)
    log_degree_ref[...] = jnp.log(mine) * LOG10E

    @pl.when(core == 1)
    def _():
        remote(degrees_sent.at[pl.ds(0, 2 * npair - 1)], deg_sem.at[0], deg_sem.at[1], dict(other=True)).wait_send()


def fit(genes_all, nleft, npower, degrees, fit_ref):
    blocks, height, genes = degrees.shape
    padded = fit_ref.shape[0] - 8

    def fold(values, combine):
        total = values[:npower]
        for block in range(1, nleft):
            total = combine(total, values[block * npower:(block + 1) * npower])
        return total

    best = degrees[0]
    for index in range(1, blocks):
        best = jnp.maximum(best, degrees[index])
    best = jnp.broadcast_to(jnp.max(best, axis=1, keepdims=True), (height, genes))
    scales = [BINS / fold(best, jnp.maximum)] * nleft
    if height > nleft * npower:
        scales.append(jnp.ones((height - nleft * npower, genes), jnp.float32))
    scale = jnp.concatenate(scales, axis=0)
    positions = [jnp.clip(degrees[index] * scale - 0.5, 0.0, BINS - 1.0) for index in range(blocks)]
    lane = lax.broadcasted_iota(jnp.int32, (height, 128), 1)
    table = jnp.zeros((height, 128), jnp.float32)
    for b in range(BINS + 1):
        total = None
        for index in range(blocks):
            term = degrees[index] if b == BINS else jnp.maximum(0.0, 1.0 - jnp.abs(positions[index] - b))
            total = term if total is None else total + term
        table = jnp.where(lane == b, jnp.sum(total, axis=1, keepdims=True), table)
    table = fold(table, jnp.add) / genes_all
    fit_ref[0:npower, :] = table
    lane = lax.broadcasted_iota(jnp.int32, (npower, 128), 1)
    line = lax.broadcasted_iota(jnp.int32, (npower, 128), 0)
    logs = [math.log10(b + 0.5) for b in range(BINS)]
    deviations = [value - sum(logs) / BINS for value in logs]
    square = sum(value * value for value in deviations)
    xdev = jnp.zeros((npower, 128), jnp.float32)
    for b in range(BINS):
        xdev = jnp.where(lane == b, deviations[b] / square, xdev)
    yfit = jnp.log(jnp.where(lane < BINS, table + 1.0 / genes_all, 1.0)) * LOG10E
    slope = jnp.sum(xdev * yfit, axis=1, keepdims=True)
    total = jnp.sum(jnp.where(lane == BINS, table, 0.0), axis=1, keepdims=True)
    mean_log = jnp.log(total) * LOG10E
    fit_ref[padded:padded + 1, :] = jnp.sum(jnp.where(lane == line, slope, 0.0), axis=0, keepdims=True)
    fit_ref[padded + 1:padded + 2, :] = jnp.sum(jnp.where(lane == line, mean_log, 0.0), axis=0, keepdims=True)


def unpack_kernel(npower, log_degree_in, fit_in, log_degree_ref, freq_ref, slope_ref, mean_log_ref):
    padded = fit_in.shape[0] - 8
    log_degree_ref[...] = log_degree_in[...]
    freq_ref[...] = fit_in[0:npower, :BINS]
    slope_ref[...] = fit_in[padded:padded + 1, :npower]
    mean_log_ref[...] = fit_in[padded + 1:padded + 2, :npower]


def solution(mesh):
    nr, nc = mesh.shape["row"], mesh.shape["col"]
    n1, n0 = split(nr // 2)
    nh, nl = split(nc)

    def on_device(expression, powers):
        genes, samples = expression.shape
        npower = powers.shape[0]
        nleft, npair = nh * n0, nl * n1
        height = -(-2 * npower * nleft // 8) * 8
        vmem = pl.BlockSpec(memory_space=pltpu.VMEM)
        hbm = pl.BlockSpec(memory_space=pltpu.HBM)
        dma = pltpu.SemaphoreType.DMA
        f32 = jnp.float32
        padded = npower + 8 - npower % 8
        log_degree, packed = pl.pallas_call(
            functools.partial(kernel, n0, n1, nh, nl, npower),
            out_shape=(
                pltpu.VMEM((npower, genes), f32),
                pltpu.VMEM((padded + 8, 128), f32),
            ),
            in_specs=[hbm, hbm],
            out_specs=(vmem, vmem),
            scratch_shapes=[
                pltpu.SMEM((npower,), jnp.int32),
                pltpu.VMEM((nleft, genes, samples), jnp.bfloat16),
                pltpu.VMEM((npair, 2 * genes, samples), jnp.bfloat16),
                pltpu.VMEM((nleft + 2 * npair, 2, genes), f32),
                pltpu.VMEM((npair, 2 * genes, 128), f32),
                pltpu.VMEM((npair, 2 * genes, 128), f32),
                pltpu.VMEM((nleft, npair, 2 * genes, genes), f32),
                pltpu.VMEM((nleft, npower, 8, genes), f32),
                pltpu.VMEM((2 * nleft * nleft, npower, genes), f32),
                pltpu.VMEM((npair, height, genes), f32),
                pltpu.VMEM((2 * npair - 1, height, genes), f32),
                dma((4,)),
                dma((3,)),
                dma((nh - 1, CHUNKS)),
                dma((nh, n0 - 1)),
                dma((nl - 1, CHUNKS)),
                dma((nl, n1 - 1, CHUNKS)),
                dma((nl, n1, 2)),
                dma((nleft + 2 * npair - 2,)),
                dma((3,)),
                dma((2,)),
            ],
            compiler_params=pltpu.CompilerParams(
                collective_id=0, has_side_effects=True, vmem_limit_bytes=67043328 - 128 * 1024
            ),
        )(powers, expression)
        log_degree, freq, slope, mean_log = pl.pallas_call(
            functools.partial(unpack_kernel, npower),
            out_shape=(
                jax.ShapeDtypeStruct((npower, genes), f32),
                jax.ShapeDtypeStruct((npower, BINS), f32),
                jax.ShapeDtypeStruct((1, npower), f32),
                jax.ShapeDtypeStruct((1, npower), f32),
            ),
            in_specs=[vmem, vmem],
            out_specs=(vmem,) * 4,
            compiler_params=pltpu.CompilerParams(vmem_limit_bytes=1 << 20),
        )(log_degree, packed)
        return log_degree, freq, slope.reshape(npower), mean_log.reshape(npower)

    return jax.shard_map(
        on_device,
        mesh=mesh,
        in_specs=(P(("row", "col"), None), P()),
        out_specs=(P(None, ("row", "col")), P(), P(), P()),
        check_vma=False,
    )
```
